32 devices in a mesh: gx: 4 (over x, core), gy: 8 (over z, y).
Axes of the slice: x: 2, y: 2, z: 4, core: 2. Of those that a mesh axis runs over, the one named last changes fastest.
Arguments:
- populations: float32 [19, 64, 4096], P(None, 'gx', 'gy'), may hold values from 0.5 to 1.5
- tracer: float32 [7, 64, 4096], P(None, 'gx', 'gy'), may hold values from 0.2 to 2
- solid_mask: int32 [64, 4096], P('gx', 'gy'), may hold values 0 or 1
- inflow: int32 [64, 4096], P('gx', 'gy'), may hold values 0 or 1
- wind_profile: float32 [3, 32], replicated, may hold values from -0.12 to 0.12
- emission: float32 [64, 4096], P('gx', 'gy'), may hold values from 0.05 to 0.5
Outputs:
- final_populations: float32 [19, 64, 4096], P(None, 'gx', 'gy')
- final_tracer: float32 [7, 64, 4096], P(None, 'gx', 'gy')
The draws below stay inside these ranges and needn't reach their ends.
All inputs are finite; a program needn't handle non-finite values. No bound on the sum of `solid_mask` or of `inflow` on one device may be relied on, other than what follows from the above.
Results may differ from the reference program's by a relative error of at most 0.0001.
Values sent between devices are 32-bit elements; how exact they have to be, the bound alone decides.
No kernel may reach another device: no remote copies, remote signals or barrier semaphores. Data moves between devices by JAX's collectives and lax.ppermute only.
A program may use at most 64 MiB of HBM per device.

```python
import math
import jax
import jax.numpy as jnp
from jax import lax

NZ = 32
STEPS = 4
NX = 64
NY = 128


def with_ends(entries, stream_key, low, top_value):
    shape = entries.shape
    index_at = [jax.random.randint(jax.random.fold_in(stream_key, axis), (), 0, shape[axis]) for axis in range(len(shape))]
    entries = entries.at[tuple(index_at)].set(low)
    longest = shape.index(max(shape))
    index_at[longest] = (index_at[longest] + 1) % shape[longest]
    return entries.at[tuple(index_at)].set(top_value)


def shard_levels(key, dims, split, least, high):
    def one(position, blocks):
        heights = jax.random.uniform(jax.random.fold_in(jax.random.fold_in(key, 6), position), (blocks,), jnp.float32, least / len(split), high / len(split))
        return jnp.repeat(jnp.exp(heights), dims[position] // blocks).reshape((-1,) + (1,) * (len(dims) - position - 1))

    level = one(*split[0])
    for cut in split[1:]:
        level = level * one(*cut)
    return level


def setup_inputs(seed: int = 0) -> dict:
    arg_keys = jax.random.split(jax.random.key(seed), 7)
    return {
        "populations": jnp.clip(0.5 + 1.0 * jax.random.uniform(arg_keys[0], (19, NX, NY * NZ), jnp.float32) ** shard_levels(arg_keys[0], (19, NX, NY * NZ), ((1, 4), (2, 8)), -0.2, 0.2), 0.5, 1.5),
        "tracer": jnp.clip(jnp.exp(math.log(2.0) - 2.3025851 * jax.random.uniform(arg_keys[1], (7, NX, NY * NZ), jnp.float32) ** shard_levels(arg_keys[1], (7, NX, NY * NZ), ((1, 4), (2, 8)), -0.2, 0.2)), 0.2, 2.0),
        "solid_mask": with_ends((jax.random.randint(arg_keys[2], (NX, NY * NZ), 0, 5) < 1).astype(jnp.int32), jax.random.fold_in(arg_keys[2], 1), 0, 1),
        "inflow": with_ends((jax.random.randint(arg_keys[3], (NX, NY * NZ), 0, 8) < 1).astype(jnp.int32), jax.random.fold_in(arg_keys[3], 1), 0, 1),
        "wind_profile": jnp.clip(jax.random.uniform(arg_keys[4], (3, NZ), jnp.float32, -0.12, 0.12), -0.12, 0.12),
        "emission": jnp.clip(jnp.exp(math.log(0.5) - 2.3025851 * jax.random.uniform(arg_keys[5], (NX, NY * NZ), jnp.float32) ** shard_levels(arg_keys[5], (NX, NY * NZ), ((0, 4), (1, 8)), -0.2, 0.2)), 0.05, 0.5),
    }


LATTICE = ((0, 0, 0), (1, 0, 0), (-1, 0, 0), (0, 1, 0), (0, -1, 0), (0, 0, 1), (0, 0, -1), (1, 1, 0), (-1, -1, 0), (1, -1, 0), (-1, 1, 0), (1, 0, 1), (-1, 0, -1), (1, 0, -1), (-1, 0, 1), (0, 1, 1), (0, -1, -1), (0, 1, -1), (0, -1, 1))
OPPOSITE = (0, 2, 1, 4, 3, 6, 5, 8, 7, 10, 9, 12, 11, 14, 13, 16, 15, 18, 17)
WEIGHTS = (1.0 / 3.0,) + (1.0 / 18.0,) * 6 + (1.0 / 36.0,) * 12
TRACER_LATTICE = LATTICE[:7]
TRACER_OPPOSITE = OPPOSITE[:7]
TRACER_WEIGHTS = (0.25,) + (0.125,) * 6
BASE_RELAX = 0.6
SMAGORINSKY = 0.2
TRACER_RELAX = 0.7

def projection(index, speed, lattice):
    return sum((lattice[index][axis] * speed[axis] for axis in range(3) if lattice[index][axis] != 0))

def equilibrium(rate, speed, speed_sq, index):
    along = projection(index, speed, LATTICE)
    return rate + 3.0 * along + 4.5 * along * along - 1.5 * speed_sq

def collide(populations, tracer, solid_mask, inflow, wind_profile, emission):
    width = populations.shape[2]
    wind_cells = jnp.tile(wind_profile, (1, width // wind_profile.shape[1]))[:, None, :]
    normal = [populations[k] for k in range(19)]
    density = sum((WEIGHTS[k] * normal[k] for k in range(19)))
    velocity = [sum((WEIGHTS[k] * LATTICE[k][axis] * normal[k] for k in range(19) if LATTICE[k][axis] != 0)) for axis in range(3)]
    speed_sq = velocity[0] * velocity[0] + velocity[1] * velocity[1] + velocity[2] * velocity[2]
    deviation = [normal[k] - equilibrium(density, velocity, speed_sq, k) for k in range(19)]
    contraction = 0.0
    for first in range(3):
        for second in range(first, 3):
            stress = sum((WEIGHTS[k] * LATTICE[k][first] * LATTICE[k][second] * deviation[k] for k in range(19) if LATTICE[k][first] * LATTICE[k][second] != 0))
            factor = 1.0 if first == second else 2.0
            contraction = contraction + factor * stress * stress
    relax_time = 0.5 * (BASE_RELAX + jnp.sqrt(BASE_RELAX * BASE_RELAX + 18.0 * math.sqrt(2.0) * SMAGORINSKY * SMAGORINSKY * jnp.sqrt(contraction)))
    wind_sq = wind_cells[0] * wind_cells[0] + wind_cells[1] * wind_cells[1] + wind_cells[2] * wind_cells[2]
    is_solid = solid_mask == 1
    is_inflow = inflow == 1
    relaxed = []
    for k in range(19):
        held = equilibrium(1.0, wind_cells, wind_sq, k)
        fluid = normal[k] - deviation[k] / relax_time
        relaxed.append(jnp.where(is_solid, normal[OPPOSITE[k]], jnp.where(is_inflow, held, fluid)))
    amount = [tracer[k] for k in range(7)]
    concentration = sum((TRACER_WEIGHTS[k] * amount[k] for k in range(7)))
    traced = []
    for k in range(7):
        balance = concentration * (1.0 + 4.0 * projection(k, velocity, TRACER_LATTICE))
        updated = amount[k] - (amount[k] - balance) / TRACER_RELAX + emission
        traced.append(jnp.where(is_solid, amount[TRACER_OPPOSITE[k]], jnp.where(is_inflow, 0.0, updated)))
    return (jnp.stack(relaxed), jnp.stack(traced))

def stream(relaxed, lattice, opposite):
    number = relaxed.shape[0]
    lattice_grid = relaxed.reshape(number, NX, NY, NZ)
    z_index = lax.iota(jnp.int32, NZ)
    layers = []
    for k in range(number):
        step_x, step_y, step_z = lattice[k]
        shifted = jnp.roll(lattice_grid[k], (step_x, step_y, step_z), axis=(0, 1, 2))
        if step_z == 1:
            shifted = jnp.where(z_index >= 1, shifted, lattice_grid[opposite[k]])
        elif step_z == -1:
            shifted = jnp.where(z_index <= NZ - 2, shifted, lattice_grid[opposite[k]])
        layers.append(shifted)
    return jnp.stack(layers).reshape(number, NX, NY * NZ)

def reference(populations, tracer, solid_mask, inflow, wind_profile, emission):
    for iteration in range(STEPS):
        relaxed, traced = collide(populations, tracer, solid_mask, inflow, wind_profile, emission)
        populations = stream(relaxed, LATTICE, OPPOSITE)
        tracer = stream(traced, TRACER_LATTICE, TRACER_OPPOSITE)
    return (populations, tracer)
```

```python
import math

import jax
import jax.numpy as jnp
from jax import lax
from jax.experimental import pallas as pl
from jax.experimental.pallas import tpu as pltpu
from jax.sharding import PartitionSpec as P

STEPS = 4
LANES = 128
ROWS = 8

LATTICE = (
    (0, 0, 0),
    (1, 0, 0),
    (-1, 0, 0),
    (0, 1, 0),
    (0, -1, 0),
    (0, 0, 1),
    (0, 0, -1),
    (1, 1, 0),
    (-1, -1, 0),
    (1, -1, 0),
    (-1, 1, 0),
    (1, 0, 1),
    (-1, 0, -1),
    (1, 0, -1),
    (-1, 0, 1),
    (0, 1, 1),
    (0, -1, -1),
    (0, 1, -1),
    (0, -1, 1),
)
OPPOSITE = (0, 2, 1, 4, 3, 6, 5, 8, 7, 10, 9, 12, 11, 14, 13, 16, 15, 18, 17)
BASE_RELAX = 0.6
SMAGORINSKY = 0.2
TRACER_RELAX = 0.7

FLOW = 19
MOVING = 26
SOLID, INFLOW, EMISSION = 26, 27, 28
UNITS = 29
SPEED = LATTICE + LATTICE[:7] + ((0, 0, 0),) * 3
TURNED = OPPOSITE + tuple(FLOW + k for k in OPPOSITE[:7])


def split_units(axis, sign):
    along = [u for u in range(UNITS) if SPEED[u][axis] == sign]
    still = [u for u in range(UNITS) if SPEED[u][axis] == 0]
    against = [u for u in range(UNITS) if SPEED[u][axis] == -sign]
    return along, still, against


def wall_pair(axis, sign):
    against = split_units(axis, sign)[2]
    return tuple(next(u for u in against if SPEED[u][2] == step) for step in (-1, 1))


def row_plan(sign):
    plan, offset = [], 0
    for units, depth in zip(split_units(0, sign), (STEPS, STEPS - 1, STEPS - 2)):
        for u in units:
            plan.append((u, STEPS - depth if sign > 0 else 0, depth, offset))
            offset += depth
    return plan, (offset, 1 if sign > 0 else 2), -(-(offset + 1) // ROWS) * ROWS


def pack_rows(read, store, sign, first, height):
    plan, (offset, row), _ = row_plan(sign)
    for u, low, depth, at in plan:
        store(at, depth, read(u, first + low, depth))
    floor, roof = wall_pair(0, sign)
    store(offset, 1, jnp.where(height[:1] == 0, read(floor, first + row, 1), read(roof, first + row, 1)))


def unpack_rows(read, store, sign, first):
    plan, (offset, row), _ = row_plan(sign)
    for u, low, depth, at in plan:
        store(u, first + low, read(at, depth))
    for u in wall_pair(0, sign):
        store(u, first + row, read(offset, 1))


def pack_columns(read, store, sign, lane, nz):
    along, still, against = split_units(1, sign)
    for t, u in enumerate(along):
        store(t, read(u))
    half = LANES // 2
    for t, u in enumerate(still):
        value = read(u)
        if t < 2 * len(against):
            chunk = t % 2
            other = read(against[t // 2])
            if sign > 0:
                value = jnp.where(lane < nz, pltpu.roll(other, half - nz * chunk, 1), value)
            else:
                value = jnp.where(lane >= LANES - nz, pltpu.roll(other, LANES - nz - nz * chunk, 1), value)
        elif t == 2 * len(against):
            floor, roof = wall_pair(1, sign)
            other = jnp.where(lane % nz == 0, read(floor), read(roof))
            if sign > 0:
                value = jnp.where(lane < nz, pltpu.roll(other, LANES - nz, 1), value)
            else:
                value = jnp.where(lane >= LANES - nz, pltpu.roll(other, nz, 1), value)
        store(len(along) + t, value)


def unpack_columns(read, store, sign, lane, nz):
    along, still, against = split_units(1, sign)
    for t, u in enumerate(along):
        store(u, read(t))
    base = len(along)
    for t, u in enumerate(still):
        store(u, read(base + t))
    half = LANES // 2
    for t, u in enumerate(against):
        first, second = read(base + 2 * t), read(base + 2 * t + 1)
        if sign > 0:
            value = jnp.where(lane < LANES - nz, pltpu.roll(first, half, 1), pltpu.roll(second, half + nz, 1))
        else:
            value = jnp.where(lane < nz, pltpu.roll(first, nz, 1), pltpu.roll(second, 2 * nz, 1))
        if u in wall_pair(1, sign):
            walls = read(base + 2 * len(against))
            if sign > 0:
                value = jnp.where(lane < half, pltpu.roll(walls, nz, 1), value)
            else:
                value = jnp.where(lane >= half, pltpu.roll(walls, LANES - nz, 1), value)
        store(u, value)


def relax(h, q, solid, inflow, emission, wind):
    w_rest, w_axis, w_diag = 1.0 / 3.0, 1.0 / 18.0, 1.0 / 36.0
    total = {k: h[k] + h[k + 1] for k in range(1, 19, 2)}
    gap = {k: h[k] - h[k + 1] for k in range(1, 19, 2)}
    xy, xz, yz = total[7] + total[9], total[11] + total[13], total[15] + total[17]
    axes = total[1] + total[3] + total[5]
    density = w_rest * h[0] + w_axis * axes + w_diag * (xy + xz + yz)
    ux = w_axis * gap[1] + w_diag * (gap[7] + gap[9] + gap[11] + gap[13])
    uy = w_axis * gap[3] + w_diag * (gap[7] - gap[9] + gap[15] + gap[17])
    uz = w_axis * gap[5] + w_diag * (gap[11] - gap[13] + gap[15] - gap[17])
    uxx, uyy, uzz = ux * ux, uy * uy, uz * uz
    third = w_rest * density
    pxx = w_axis * total[1] + w_diag * (xy + xz) - third - uxx
    pyy = w_axis * total[3] + w_diag * (xy + yz) - third - uyy
    pzz = w_axis * total[5] + w_diag * (xz + yz) - third - uzz
    pxy = w_diag * (total[7] - total[9]) - ux * uy
    pxz = w_diag * (total[11] - total[13]) - ux * uz
    pyz = w_diag * (total[15] - total[17]) - uy * uz
    cross = pxy * pxy + pxz * pxz + pyz * pyz
    contraction = pxx * pxx + pyy * pyy + pzz * pzz + (cross + cross)
    strength = 18.0 * math.sqrt(2.0) * SMAGORINSKY * SMAGORINSKY
    relax_time = 0.5 * (BASE_RELAX + jnp.sqrt(BASE_RELAX * BASE_RELAX + strength * jnp.sqrt(contraction)))
    rate = 1.0 / relax_time

    keep = 1.0 - 1.0 / TRACER_RELAX
    amount = 0.25 * q[0] + 0.125 * ((q[1] + q[2]) + (q[3] + q[4]) + (q[5] + q[6]))
    source = jnp.where(inflow, 0.0, amount * (1.0 / TRACER_RELAX))
    hold = jnp.where(inflow, 0.0, keep)
    level = source + jnp.where(inflow, 0.0, emission)
    push = 4.0 * source
    traced = [None] * 7
    traced[0] = jnp.where(solid, q[0], hold * q[0] + level)
    for k, speed in ((1, ux), (3, uy), (5, uz)):
        shift = push * speed
        traced[k] = jnp.where(solid, q[k + 1], hold * q[k] + (level + shift))
        traced[k + 1] = jnp.where(solid, q[k], hold * q[k + 1] + (level - shift))

    rate = jnp.where(inflow, 1.0, rate)
    density = jnp.where(inflow, 1.0, density)
    ux, uy, uz = (jnp.where(inflow, w, u) for w, u in zip(wind, (ux, uy, uz)))
    rest = 1.0 - rate
    square = ux * ux + uy * uy + uz * uz
    base = rate * (density - 1.5 * square)
    linear = 3.0 * rate
    quadratic = 4.5 * rate
    relaxed = [None] * 19
    relaxed[0] = jnp.where(solid, h[0], rest * h[0] + base)
    along = {1: ux, 3: uy, 5: uz, 7: ux + uy, 9: ux - uy, 11: ux + uz, 13: ux - uz, 15: uy + uz, 17: uy - uz}
    for k, speed in along.items():
        even = base + quadratic * speed * speed
        odd = linear * speed
        relaxed[k] = jnp.where(solid, h[k + 1], rest * h[k] + (even + odd))
        relaxed[k + 1] = jnp.where(solid, h[k], rest * h[k + 1] + (even - odd))
    return relaxed + traced


def lane_index():
    return lax.broadcasted_iota(jnp.int32, (ROWS, LANES), 1)


def wind_tiles(wind, nz):
    row = jnp.concatenate([wind[...]] * (LANES // nz), axis=1)
    return [jnp.broadcast_to(row[a : a + 1], (ROWS, LANES)) for a in range(3)]


def first_step(populations, tracer, solid, inflow, wind, emission, centre, y_up, y_down, x_up, x_down):
    extent = populations.shape[1]
    tiles = populations.shape[2] // LANES
    nz = wind.shape[1]
    winds = wind_tiles(wind, nz)
    lane = lane_index()
    height = lane % nz
    for j in range(tiles):
        lanes = slice(j * LANES, (j + 1) * LANES)
        for r in range(0, extent, ROWS):
            rows = slice(r, r + ROWS)
            h = [populations[k, rows, lanes] for k in range(FLOW)]
            q = [tracer[k, rows, lanes] for k in range(7)]
            built, held, emitted = solid[rows, lanes], inflow[rows, lanes], emission[rows, lanes]
            out = relax(h, q, built == 1, held == 1, emitted, winds)
            out += [built.astype(jnp.float32), held.astype(jnp.float32), emitted]
            for u in range(UNITS):
                centre[u, j, rows, :] = out[u]
        for sign, target, first in ((1, x_up, extent - STEPS), (-1, x_down, 0)):
            def store(offset, depth, value, target=target, j=j):
                target[j, offset : offset + depth, :] = value

            pack_rows(lambda u, low, depth, j=j: centre[u, j, low : low + depth, :], store, sign, first, height)
    for sign, target, j in ((1, y_up, tiles - 1), (-1, y_down, 0)):
        for r in range(0, extent, ROWS):
            rows = slice(r, r + ROWS)

            def store(t, value, target=target, rows=rows):
                target[t, rows, :] = value

            pack_columns(lambda u, j=j, rows=rows: centre[u, j, rows, :], store, sign, lane, nz)


def turn_corner(nz, from_south, from_north, sides, x_up, x_down):
    extent = sides.shape[2]
    lane = lane_index()
    height = lane % nz
    for side, (sign, source) in enumerate(((1, from_south), (-1, from_north))):
        for r in range(0, extent, ROWS):
            rows = slice(r, r + ROWS)

            def store(u, value, side=side, rows=rows):
                sides[u, side, rows, :] = value

            unpack_columns(lambda t, source=source, rows=rows: source[t, rows, :], store, sign, lane, nz)
        for sign_x, target, first in ((1, x_up, extent - STEPS), (-1, x_down, 0)):
            def put(offset, depth, value, target=target, side=side):
                target[side, offset : offset + depth, :] = value

            pack_rows(lambda u, low, depth, side=side: sides[u, side, low : low + depth, :], put, sign_x, first, height)


def later_steps(centre, sides, wind, west, east, corner_west, corner_east, flow_out, tracer_out, grown, ping, pong):
    tiles, extent = centre.shape[1], centre.shape[2]
    wide = tiles + 2
    nz = wind.shape[1]
    winds = wind_tiles(wind, nz)
    lane = lane_index()
    height = lane % nz
    for u in range(UNITS):
        for j in range(wide):
            for r in range(0, extent, ROWS):
                if j == 0:
                    value = sides[u, 0, r : r + ROWS, :]
                elif j == wide - 1:
                    value = sides[u, 1, r : r + ROWS, :]
                else:
                    value = centre[u, j - 1, r : r + ROWS, :]
                grown[u, j, STEPS + r : STEPS + r + ROWS, :] = value
    for j in range(wide):
        inner = 1 <= j <= tiles
        at = j - 1 if inner else (0 if j == 0 else 1)
        for sign, source, first in (
            (1, west if inner else corner_west, 0),
            (-1, east if inner else corner_east, STEPS + extent),
        ):

            def fill(u, row, value, j=j):
                grown[u, j, row : row + value.shape[0], :] = value

            unpack_rows(
                lambda offset, depth, source=source, at=at: source[at, offset : offset + depth, :], fill, sign, first
            )

    def pulled(buffer, u, j, before, after, r):
        step_x, step_y, step_z = SPEED[u]
        rows = pl.ds(r - step_x, ROWS)
        value = buffer[u, j, rows, :]
        if step_y == 1:
            value = jnp.where(lane >= LANES - nz, buffer[u, before, rows, :], value)
        elif step_y == -1:
            value = jnp.where(lane < nz, buffer[u, after, rows, :], value)
        shift = (nz * step_y + step_z) % LANES
        if shift:
            value = pltpu.roll(value, shift, 1)
        if step_z:
            edge = height == (0 if step_z == 1 else nz - 1)
            value = jnp.where(edge, buffer[TURNED[u], j, pl.ds(r, ROWS), :], value)
        return value

    source = grown
    for step in range(1, STEPS):
        target = ping if step % 2 else pong
        low, high = step, extent + 2 * STEPS - step
        firsts = list(range(low, high - ROWS, ROWS)) + [high - ROWS]

        def column(j, _, source=source, target=target, firsts=firsts):
            before, after = jnp.maximum(j - 1, 0), jnp.minimum(j + 1, wide - 1)
            for r in firsts:
                moved = [pulled(source, u, j, before, after, r) for u in range(MOVING)]
                cells = pl.ds(r, ROWS)
                out = relax(
                    moved[:FLOW],
                    moved[FLOW:],
                    grown[SOLID, j, cells, :] == 1.0,
                    grown[INFLOW, j, cells, :] == 1.0,
                    grown[EMISSION, j, cells, :],
                    winds,
                )
                for u in range(MOVING):
                    target[u, j, cells, :] = out[u]
            return _

        lax.fori_loop(0, wide, column, 0)
        source = target
    for j in range(1, tiles + 1):
        lanes = slice((j - 1) * LANES, j * LANES)
        for r in range(0, extent, ROWS):
            for u in range(MOVING):
                value = pulled(source, u, j, j - 1, j + 1, STEPS + r)
                if u < FLOW:
                    flow_out[u, r : r + ROWS, lanes] = value
                else:
                    tracer_out[u - FLOW, r : r + ROWS, lanes] = value


def passed_along(shard, axis, by):
    length = lax.axis_size(axis)
    return lax.ppermute(shard, axis, [(i, (i + by) % length) for i in range(length)])


def near(x):
    return pltpu.with_memory_space_constraint(x, pltpu.VMEM)


def local(populations, tracer, solid_mask, inflow, wind_profile, emission):
    extent = populations.shape[1]
    tiles = populations.shape[2] // LANES
    nz = wind_profile.shape[1]
    along, still, _ = split_units(1, 1)
    messages = len(along) + len(still)
    packed = row_plan(1)[2]
    vm = lambda *shape: pltpu.VMEM(shape, jnp.float32)
    plain = lambda *shape: jax.ShapeDtypeStruct(shape, jnp.float32)
    centre, y_up, y_down, x_up, x_down = pl.pallas_call(
        first_step,
        out_shape=(
            vm(UNITS, tiles, extent, LANES),
            vm(messages, extent, LANES),
            vm(messages, extent, LANES),
            vm(tiles, packed, LANES),
            vm(tiles, packed, LANES),
        ),
        name="first_step",
    )(populations, tracer, solid_mask, inflow, wind_profile, emission)
    from_south = passed_along(y_up, "gy", 1)
    from_north = passed_along(y_down, "gy", -1)
    west = passed_along(x_up, "gx", 1)
    east = passed_along(x_down, "gx", -1)
    sides, corner_up, corner_down = pl.pallas_call(
        lambda *refs: turn_corner(nz, *refs),
        out_shape=(vm(UNITS, 2, extent, LANES), vm(2, packed, LANES), vm(2, packed, LANES)),
        name="turn_corner",
    )(near(from_south), near(from_north))
    corner_west = passed_along(corner_up, "gx", 1)
    corner_east = passed_along(corner_down, "gx", -1)
    rows = extent + 2 * STEPS
    return pl.pallas_call(
        later_steps,
        out_shape=(plain(FLOW, extent, tiles * LANES), plain(7, extent, tiles * LANES)),
        scratch_shapes=[
            vm(UNITS, tiles + 2, rows, LANES),
            vm(MOVING, tiles + 2, rows, LANES),
            vm(MOVING, tiles + 2, rows, LANES),
        ],
        name="later_steps",
    )(near(centre), near(sides), wind_profile, near(west), near(east), near(corner_west), near(corner_east))


def solution(mesh):
    in_specs = (
        P(None, "gx", "gy"),
        P(None, "gx", "gy"),
        P("gx", "gy"),
        P("gx", "gy"),
        P(),
        P("gx", "gy"),
    )
    out_specs = (P(None, "gx", "gy"), P(None, "gx", "gy"))
    return jax.shard_map(local, mesh=mesh, in_specs=in_specs, out_specs=out_specs, check_vma=False)
```

```python
import math

import jax
import jax.numpy as jnp
from jax import lax
from jax.experimental import pallas as pl
from jax.experimental.pallas import tpu as pltpu
from jax.sharding import PartitionSpec as P


STEPS = 4
LANES = 128
KERNEL_BYTES = 16 * 2**20
ROWS = 8

LATTICE = (
    (0, 0, 0),
    (1, 0, 0),
    (-1, 0, 0),
    (0, 1, 0),
    (0, -1, 0),
    (0, 0, 1),
    (0, 0, -1),
    (1, 1, 0),
    (-1, -1, 0),
    (1, -1, 0),
    (-1, 1, 0),
    (1, 0, 1),
    (-1, 0, -1),
    (1, 0, -1),
    (-1, 0, 1),
    (0, 1, 1),
    (0, -1, -1),
    (0, 1, -1),
    (0, -1, 1),
)
OPPOSITE = (0, 2, 1, 4, 3, 6, 5, 8, 7, 10, 9, 12, 11, 14, 13, 16, 15, 18, 17)
BASE_RELAX = 0.6
SMAGORINSKY = 0.2
TRACER_RELAX = 0.7

FLOW = 19
MOVING = 26
SOLID, INFLOW, EMISSION = 26, 27, 28
UNITS = 29
SPEED = LATTICE + LATTICE[:7] + ((0, 0, 0),) * 3
TURNED = OPPOSITE + tuple(FLOW + k for k in OPPOSITE[:7])


def split_units(axis, sign):
    along = [u for u in range(UNITS) if SPEED[u][axis] == sign]
    still = [u for u in range(UNITS) if SPEED[u][axis] == 0]
    against = [u for u in range(UNITS) if SPEED[u][axis] == -sign]
    return along, still, against


def wall_pair(axis, sign):
    against = split_units(axis, sign)[2]
    return tuple(next(u for u in against if SPEED[u][2] == step) for step in (-1, 1))


def row_plan(sign):
    plan, offset = [], 0
    for units, depth in zip(split_units(0, sign), (STEPS, STEPS - 1, STEPS - 2)):
        for u in units:
            plan.append((u, STEPS - depth if sign > 0 else 0, depth, offset))
            offset += depth
    return plan, (offset, 1 if sign > 0 else 2), -(-(offset + 1) // ROWS) * ROWS


def pack_rows(read, store, sign, first, height):
    plan, (offset, row), _ = row_plan(sign)
    for u, low, depth, at in plan:
        store(at, depth, read(u, first + low, depth))
    floor, roof = wall_pair(0, sign)
    store(offset, 1, jnp.where(height[:1] == 0, read(floor, first + row, 1), read(roof, first + row, 1)))


def unpack_rows(read, store, sign, first):
    plan, (offset, row), _ = row_plan(sign)
    for u, low, depth, at in plan:
        store(u, first + low, read(at, depth))
    for u in wall_pair(0, sign):
        store(u, first + row, read(offset, 1))


def pack_columns(read, store, sign, lane, nz):
    along, still, against = split_units(1, sign)
    for t, u in enumerate(along):
        store(t, read(u))
    half = LANES // 2
    for t, u in enumerate(still):
        value = read(u)
        if t < 2 * len(against):
            chunk = t % 2
            other = read(against[t // 2])
            if sign > 0:
                value = jnp.where(lane < nz, pltpu.roll(other, half - nz * chunk, 1), value)
            else:
                value = jnp.where(lane >= LANES - nz, pltpu.roll(other, LANES - nz - nz * chunk, 1), value)
        elif t == 2 * len(against):
            floor, roof = wall_pair(1, sign)
            other = jnp.where(lane % nz == 0, read(floor), read(roof))
            if sign > 0:
                value = jnp.where(lane < nz, pltpu.roll(other, LANES - nz, 1), value)
            else:
                value = jnp.where(lane >= LANES - nz, pltpu.roll(other, nz, 1), value)
        store(len(along) + t, value)


def unpack_columns(read, store, sign, lane, nz):
    along, still, against = split_units(1, sign)
    for t, u in enumerate(along):
        store(u, read(t))
    base = len(along)
    for t, u in enumerate(still):
        store(u, read(base + t))
    half = LANES // 2
    for t, u in enumerate(against):
        first, second = read(base + 2 * t), read(base + 2 * t + 1)
        if sign > 0:
            value = jnp.where(lane < LANES - nz, pltpu.roll(first, half, 1), pltpu.roll(second, half + nz, 1))
        else:
            value = jnp.where(lane < nz, pltpu.roll(first, nz, 1), pltpu.roll(second, 2 * nz, 1))
        if u in wall_pair(1, sign):
            walls = read(base + 2 * len(against))
            if sign > 0:
                value = jnp.where(lane < half, pltpu.roll(walls, nz, 1), value)
            else:
                value = jnp.where(lane >= half, pltpu.roll(walls, LANES - nz, 1), value)
        store(u, value)


def relax(h, q, solid, inflow, emission, wind):
    w_rest, w_axis, w_diag = 1.0 / 3.0, 1.0 / 18.0, 1.0 / 36.0
    total = {k: h[k] + h[k + 1] for k in range(1, 19, 2)}
    gap = {k: h[k] - h[k + 1] for k in range(1, 19, 2)}
    xy, xz, yz = total[7] + total[9], total[11] + total[13], total[15] + total[17]
    axes = total[1] + total[3] + total[5]
    density = w_rest * h[0] + w_axis * axes + w_diag * (xy + xz + yz)
    ux = w_axis * gap[1] + w_diag * (gap[7] + gap[9] + gap[11] + gap[13])
    uy = w_axis * gap[3] + w_diag * (gap[7] - gap[9] + gap[15] + gap[17])
    uz = w_axis * gap[5] + w_diag * (gap[11] - gap[13] + gap[15] - gap[17])
    uxx, uyy, uzz = ux * ux, uy * uy, uz * uz
    third = w_rest * density
    pxx = w_axis * total[1] + w_diag * (xy + xz) - third - uxx
    pyy = w_axis * total[3] + w_diag * (xy + yz) - third - uyy
    pzz = w_axis * total[5] + w_diag * (xz + yz) - third - uzz
    pxy = w_diag * (total[7] - total[9]) - ux * uy
    pxz = w_diag * (total[11] - total[13]) - ux * uz
    pyz = w_diag * (total[15] - total[17]) - uy * uz
    cross = pxy * pxy + pxz * pxz + pyz * pyz
    contraction = pxx * pxx + pyy * pyy + pzz * pzz + (cross + cross)
    strength = 18.0 * math.sqrt(2.0) * SMAGORINSKY * SMAGORINSKY
    relax_time = 0.5 * (BASE_RELAX + jnp.sqrt(BASE_RELAX * BASE_RELAX + strength * jnp.sqrt(contraction)))
    rate = 1.0 / relax_time

    keep = 1.0 - 1.0 / TRACER_RELAX
    amount = 0.25 * q[0] + 0.125 * ((q[1] + q[2]) + (q[3] + q[4]) + (q[5] + q[6]))
    source = jnp.where(inflow, 0.0, amount * (1.0 / TRACER_RELAX))
    hold = jnp.where(inflow, 0.0, keep)
    level = source + jnp.where(inflow, 0.0, emission)
    push = 4.0 * source
    traced = [None] * 7
    traced[0] = jnp.where(solid, q[0], hold * q[0] + level)
    for k, speed in ((1, ux), (3, uy), (5, uz)):
        shift = push * speed
        traced[k] = jnp.where(solid, q[k + 1], hold * q[k] + (level + shift))
        traced[k + 1] = jnp.where(solid, q[k], hold * q[k + 1] + (level - shift))

    rate = jnp.where(inflow, 1.0, rate)
    density = jnp.where(inflow, 1.0, density)
    ux, uy, uz = (jnp.where(inflow, w, u) for w, u in zip(wind, (ux, uy, uz)))
    rest = 1.0 - rate
    square = ux * ux + uy * uy + uz * uz
    base = rate * (density - 1.5 * square)
    linear = 3.0 * rate
    quadratic = 4.5 * rate
    relaxed = [None] * 19
    relaxed[0] = jnp.where(solid, h[0], rest * h[0] + base)
    along = {1: ux, 3: uy, 5: uz, 7: ux + uy, 9: ux - uy, 11: ux + uz, 13: ux - uz, 15: uy + uz, 17: uy - uz}
    for k, speed in along.items():
        even = base + quadratic * speed * speed
        odd = linear * speed
        relaxed[k] = jnp.where(solid, h[k + 1], rest * h[k] + (even + odd))
        relaxed[k + 1] = jnp.where(solid, h[k], rest * h[k + 1] + (even - odd))
    return relaxed + traced


def lane_index():
    return lax.broadcasted_iota(jnp.int32, (ROWS, LANES), 1)


def wind_tiles(wind):
    return [jnp.broadcast_to(wind[a : a + 1, :], (ROWS, LANES)) for a in range(3)]


def start_all(copies, sems):
    started = [pltpu.make_async_copy(src, dst, sems.at[n]) for n, (src, dst) in enumerate(copies)]
    for copy in started:
        copy.start()
    return started


def relax_own(cells, winds, store, rows):
    populations, tracer, solid, inflow, emission = cells
    h = [populations[k, rows, :] for k in range(FLOW)]
    q = [tracer[k, rows, :] for k in range(7)]
    built, held, emitted = solid[rows, :], inflow[rows, :], emission[rows, :]
    out = relax(h, q, built == 1, held == 1, emitted, winds)
    for u, value in enumerate(out + [built.astype(jnp.float32), held.astype(jnp.float32), emitted]):
        store(u, value)


def load_tiles(arrays, buffers, columns, sems, extra=()):
    copies = list(extra)
    for n, j in enumerate(columns):
        lanes = pl.ds(j * LANES, LANES)
        for array, buffer in zip(arrays, buffers):
            src = array.at[:, :, lanes] if len(array.shape) == 3 else array.at[:, lanes]
            copies.append((src, buffer.at[n]))
    started = start_all(copies, sems)
    count = len(arrays)
    own = [started[len(extra) + n * count : len(extra) + (n + 1) * count] for n in range(len(columns))]
    return started[: len(extra)], own


def first_edges(
    populations, tracer, solid, inflow, wind, emission, edge, winds, y_up, y_down,
    wind_in, pop_in, tracer_in, solid_in, inflow_in, emission_in, sems,
):
    extent = populations.shape[1]
    tiles = populations.shape[2] // LANES
    nz = wind.shape[1]
    lane = lane_index()
    buffers = (pop_in, tracer_in, solid_in, inflow_in, emission_in)
    common, own = load_tiles(
        (populations, tracer, solid, inflow, emission), buffers, (tiles - 1, 0), sems, ((wind, wind_in),)
    )
    for copy in common:
        copy.wait()
    winds[...] = jnp.concatenate([wind_in[...]] * (LANES // nz), axis=1)
    wind_values = wind_tiles(winds)
    for n, (at, sign, target) in enumerate(((1, 1, y_up), (0, -1, y_down))):
        for copy in own[n]:
            copy.wait()
        cells = [b.at[n] for b in buffers]
        for r in range(0, extent, ROWS):
            rows = slice(r, r + ROWS)

            def keep(u, value, at=at, rows=rows):
                edge[u, at, rows, :] = value

            relax_own(cells, wind_values, keep, rows)
        for r in range(0, extent, ROWS):
            rows = slice(r, r + ROWS)

            def send(t, value, target=target, rows=rows):
                target[t, rows, :] = value

            pack_columns(lambda u, at=at, rows=rows: edge[u, at, rows, :], send, sign, lane, nz)


def first_inner(
    populations, tracer, solid, inflow, emission, winds, edge, inner, x_up, x_down,
    pop_in, tracer_in, solid_in, inflow_in, emission_in, sems, *, nz,
):
    extent = populations.shape[1]
    tiles = populations.shape[2] // LANES
    height = lane_index() % nz
    buffers = (pop_in, tracer_in, solid_in, inflow_in, emission_in)
    columns = tuple(range(1, tiles - 1))
    _, own = load_tiles((populations, tracer, solid, inflow, emission), buffers, columns, sems)
    wind_values = wind_tiles(winds)

    def pack(j, source, at):
        for sign, target, first in ((1, x_up, extent - STEPS), (-1, x_down, 0)):
            def store(offset, depth, value, target=target):
                target[j, offset : offset + depth, :] = value

            pack_rows(lambda u, low, depth: source[u, at, low : low + depth, :], store, sign, first, height)

    pack(0, edge, 0)
    pack(tiles - 1, edge, 1)
    for n, j in enumerate(columns):
        for copy in own[n]:
            copy.wait()
        for r in range(0, extent, ROWS):
            rows = slice(r, r + ROWS)

            def keep(u, value, n=n, rows=rows):
                inner[u, n, rows, :] = value

            relax_own([b.at[n] for b in buffers], wind_values, keep, rows)
        pack(j, inner, n)


def turn_corner(from_south, from_north, sides, x_up, x_down, *, nz):
    extent = sides.shape[2]
    lane = lane_index()
    height = lane % nz
    for side, (sign, source) in enumerate(((1, from_south), (-1, from_north))):
        for r in range(0, extent, ROWS):
            rows = slice(r, r + ROWS)

            def store(u, value, side=side, rows=rows):
                sides[u, side, rows, :] = value

            unpack_columns(lambda t, source=source, rows=rows: source[t, rows, :], store, sign, lane, nz)
        for sign_x, target, first in ((1, x_up, extent - STEPS), (-1, x_down, 0)):
            def put(offset, depth, value, target=target, side=side):
                target[side, offset : offset + depth, :] = value

            pack_rows(lambda u, low, depth, side=side: sides[u, side, low : low + depth, :], put, sign_x, first, height)


class Mover:
    def __init__(self, nz):
        lane = lane_index()
        height = lane % nz
        self.nz = nz
        self.from_part = [None] + [lane >= part * nz for part in range(1, LANES // nz)]
        self.floor, self.roof = height == 0, height == nz - 1

    def merge(self, read, columns):
        value = read(columns[0])
        for part in range(1, len(columns)):
            if columns[part] != columns[part - 1]:
                value = jnp.where(self.from_part[part], read(columns[part]), value)
        return value

    def pull(self, read, parts, u, r):
        step_x, step_y, step_z = SPEED[u]
        value = self.merge(lambda c: read(u, c, r - step_x), parts[step_y])
        shift = (self.nz * step_y + step_z) % LANES
        if shift:
            value = pltpu.roll(value, shift, 1)
        if step_z:
            own = self.merge(lambda c: read(TURNED[u], c, r), parts[0])
            value = jnp.where(self.floor if step_z == 1 else self.roof, own, value)
        return value


def plain_parts(column, before, after, count):
    return {0: [column] * count, 1: [column] * (count - 1) + [before], -1: [after] + [column] * (count - 1)}


def row_starts(step, rows):
    low, high = step, rows - step
    return list(range(low, high - ROWS, ROWS)) + [high - ROWS]


def relax_column(mover, read, fields, parts, here, step, rows, winds, store):
    for r in row_starts(step, rows):
        moved = [mover.pull(read, parts, u, r) for u in range(MOVING)]
        solid, inflow, emission = (mover.merge(lambda c, u=u: fields(u, c, r), here) for u in (SOLID, INFLOW, EMISSION))
        out = relax(moved[:FLOW], moved[FLOW:], solid == 1.0, inflow == 1.0, emission, winds)
        for u in range(MOVING):
            store(u, r, out[u])


def inner_steps(edge, inner, winds, west, east, one, two, three, four, done, *, nz):
    tiles, rows = one.shape[1], one.shape[2]
    extent = rows - 2 * STEPS
    count = LANES // nz
    mover = Mover(nz)
    wind_values = wind_tiles(winds)
    for j in range(tiles):
        for u in range(UNITS):
            for r in range(0, extent, ROWS):
                cells = slice(r, r + ROWS)
                if j in (0, tiles - 1):
                    value = edge[u, 0 if j == 0 else 1, cells, :]
                else:
                    value = inner[u, j - 1, cells, :]
                one[u, j, STEPS + r : STEPS + r + ROWS, :] = value
        for sign, source, first in ((1, west, 0), (-1, east, STEPS + extent)):
            def fill(u, row, value, j=j):
                one[u, j, row : row + value.shape[0], :] = value

            unpack_rows(
                lambda offset, depth, source=source, j=j: source[j, offset : offset + depth, :], fill, sign, first
            )
    levels = (one, two, three, four)
    for step in range(1, STEPS):
        source, target = levels[step - 1], levels[step]

        def column(j, carry, source=source, target=target, step=step):
            before, after = jnp.maximum(j - 1, 0), jnp.minimum(j + 1, tiles - 1)
            names = {"here": j, "before": before, "after": after}

            def store(u, r, value):
                target[u, j, pl.ds(r, ROWS), :] = value

            relax_column(
                mover,
                lambda u, c, r: source[u, names[c], pl.ds(r, ROWS), :],
                lambda u, c, r: one[u, names[c], pl.ds(r, ROWS), :],
                plain_parts("here", "before", "after", count),
                ["here"] * count,
                step,
                rows,
                wind_values,
                store,
            )
            return carry

        lax.fori_loop(0, tiles, column, 0)
    for j in range(1, tiles - 1):
        for r in range(0, extent, ROWS):
            for u in range(MOVING):
                done[u, j - 1, r : r + ROWS, :] = mover.pull(
                    lambda u, c, at: four[u, c, at : at + ROWS, :], plain_parts(j, j - 1, j + 1, count), u, STEPS + r
                )


def outer_steps(
    one, two, three, four, done, winds, sides, corner_west, corner_east, flow_out, tracer_out,
    margin, outer_two, outer_three, outer_four, edge_done, sems, *, nz,
):
    tiles, rows = one.shape[1], one.shape[2]
    extent = rows - 2 * STEPS
    count = LANES // nz
    part = count // 2
    mover = Mover(nz)
    wind_values = wind_tiles(winds)
    last = tiles + 1
    copies = []

    def write_out(source, at, j):
        lanes = pl.ds(j * LANES, LANES)
        for units, target in (((0, FLOW), flow_out), ((FLOW, MOVING), tracer_out)):
            copy = pltpu.make_async_copy(
                source.at[pl.ds(units[0], units[1] - units[0]), at], target.at[:, :, lanes], sems.at[len(copies)]
            )
            copy.start()
            copies.append(copy)

    for j in range(1, tiles - 1):
        write_out(done, j - 1, j)
    for side in range(2):
        for u in range(UNITS):
            for r in range(0, extent, ROWS):
                margin[u, side, STEPS + r : STEPS + r + ROWS, :] = sides[u, side, r : r + ROWS, :]
        for sign_x, corner, first in ((1, corner_west, 0), (-1, corner_east, STEPS + extent)):
            def fill(u, row, value, side=side):
                margin[u, side, row : row + value.shape[0], :] = value

            unpack_rows(
                lambda offset, depth, corner=corner, side=side: corner[side, offset : offset + depth, :],
                fill,
                sign_x,
                first,
            )

    both = -1
    outer = (
        None,
        {0: (margin, 0), last: (margin, 1)},
        {0: (outer_two, 0), 1: (outer_two, 1), tiles: (outer_two, 2), last: (outer_two, 3)},
        {both: (outer_three, 2), 1: (outer_three, 0), tiles: (outer_three, 1)},
        {both: (outer_four, 2), 1: (outer_four, 0), tiles: (outer_four, 1)},
    )
    own = (None, one, two, three, four)

    def reader(level):
        def read(u, c, r):
            ref, at = outer[level].get(c, (own[level], c - 1))
            return ref[u, at, r : r + ROWS, :]

        return read

    def parts_of(level, c):
        if c == both and level == 2:
            return {
                0: [last] * part + [0] * (count - part),
                1: [last] * (part - 1) + [0] * (count - part) + [tiles],
                -1: [1] + [last] * part + [0] * (count - part - 1),
            }
        if c == both:
            return plain_parts(both, tiles, 1, count)
        before = both if c == 1 and level > 2 else max(c - 1, 0)
        after = both if c == tiles and level > 2 else min(c + 1, last)
        return plain_parts(c, before, after, count)

    for step in range(1, STEPS):
        for c, (target, at) in outer[step + 1].items():
            def store(u, r, value, target=target, at=at):
                target[u, at, r : r + ROWS, :] = value

            parts = parts_of(step, c)
            here = parts if c != both else parts_of(2, both)
            relax_column(mover, reader(step), reader(1), parts, here[0], step, rows, wind_values, store)
    for n, c in enumerate((1, tiles)):
        for r in range(0, extent, ROWS):
            for u in range(MOVING):
                edge_done[u, n, r : r + ROWS, :] = mover.pull(reader(STEPS), parts_of(STEPS, c), u, STEPS + r)
        write_out(edge_done, n, c - 1)
    for copy in copies:
        copy.wait()


def passed_along(shard, axis, by):
    length = lax.axis_size(axis)
    return lax.ppermute(shard, axis, [(i, (i + by) % length) for i in range(length)])


def local(populations, tracer, solid_mask, inflow, wind_profile, emission):
    extent = populations.shape[1]
    tiles = populations.shape[2] // LANES
    nz = wind_profile.shape[1]
    inner_tiles = tiles - 2
    along, still, _ = split_units(1, 1)
    messages = len(along) + len(still)
    packed = row_plan(1)[2]
    rows = extent + 2 * STEPS
    vm = lambda *shape: pltpu.VMEM(shape, jnp.float32)
    far = pl.BlockSpec(memory_space=pltpu.HBM)
    close = pl.BlockSpec(memory_space=pltpu.VMEM)

    def buffers(number):
        return [
            vm(number, FLOW, extent, LANES),
            vm(number, 7, extent, LANES),
            pltpu.VMEM((number, extent, LANES), jnp.int32),
            pltpu.VMEM((number, extent, LANES), jnp.int32),
            vm(number, extent, LANES),
            pltpu.SemaphoreType.DMA((5 * number + 1,)),
        ]

    def run(body, out_shape, args, far_args=0, out_specs=None, scratch=()):
        specs = [far] * far_args + [close] * (len(args) - far_args)
        args = tuple(pltpu.with_memory_space_constraint(a, pltpu.HBM if n < far_args else pltpu.VMEM) for n, a in enumerate(args))
        options = {} if out_specs is None else {"out_specs": out_specs}
        return pl.pallas_call(
            body,
            out_shape=out_shape,
            in_specs=specs,
            scratch_shapes=list(scratch),
            compiler_params=pltpu.CompilerParams(vmem_limit_bytes=KERNEL_BYTES),
            **options,
        )(*args)

    edge, winds, y_up, y_down = run(
        first_edges,
        (
            vm(UNITS, 2, extent, LANES),
            vm(3, LANES),
            vm(messages, extent, LANES),
            vm(messages, extent, LANES),
        ),
        (populations, tracer, solid_mask, inflow, wind_profile, emission),
        far_args=6,
        scratch=[vm(3, nz)] + buffers(2),
    )
    from_south = passed_along(y_up, "gy", 1)
    from_north = passed_along(y_down, "gy", -1)
    inner, x_up, x_down = run(
        lambda *refs: first_inner(*refs, nz=nz),
        (vm(UNITS, inner_tiles, extent, LANES), vm(tiles, packed, LANES), vm(tiles, packed, LANES)),
        (populations, tracer, solid_mask, inflow, emission, winds, edge),
        far_args=5,
        scratch=buffers(inner_tiles),
    )
    west = passed_along(x_up, "gx", 1)
    east = passed_along(x_down, "gx", -1)
    sides, corner_up, corner_down = run(
        lambda *refs: turn_corner(*refs, nz=nz),
        (vm(UNITS, 2, extent, LANES), vm(2, packed, LANES), vm(2, packed, LANES)),
        (from_south, from_north),
    )
    corner_west = passed_along(corner_up, "gx", 1)
    corner_east = passed_along(corner_down, "gx", -1)
    level = vm(MOVING, tiles, rows, LANES)
    one, two, three, four, done = run(
        lambda *refs: inner_steps(*refs, nz=nz),
        (vm(UNITS, tiles, rows, LANES), level, level, level, vm(MOVING, inner_tiles, extent, LANES)),
        (edge, inner, winds, west, east),
    )
    return run(
        lambda *refs: outer_steps(*refs, nz=nz),
        (
            jax.ShapeDtypeStruct((FLOW, extent, tiles * LANES), jnp.float32),
            jax.ShapeDtypeStruct((7, extent, tiles * LANES), jnp.float32),
        ),
        (one, two, three, four, done, winds, sides, corner_west, corner_east),
        out_specs=(far, far),
        scratch=[
            vm(UNITS, 2, rows, LANES),
            vm(MOVING, 4, rows, LANES),
            vm(MOVING, 3, rows, LANES),
            vm(MOVING, 3, rows, LANES),
            vm(MOVING, 2, extent, LANES),
            pltpu.SemaphoreType.DMA((2 * tiles,)),
        ],
    )


def solution(mesh):
    in_specs = (
        P(None, "gx", "gy"),
        P(None, "gx", "gy"),
        P("gx", "gy"),
        P("gx", "gy"),
        P(),
        P("gx", "gy"),
    )
    out_specs = (P(None, "gx", "gy"), P(None, "gx", "gy"))

    return jax.shard_map(local, mesh=mesh, in_specs=in_specs, out_specs=out_specs, check_vma=False)
```

```python
import math

import jax
import jax.numpy as jnp
from jax import lax
from jax.experimental import pallas as pl
from jax.experimental.pallas import tpu as pltpu
from jax.sharding import PartitionSpec as P


STEPS = 4
LANES = 128
KERNEL_BYTES = 16 * 2**20
ROWS = 8

LATTICE = (
    (0, 0, 0),
    (1, 0, 0),
    (-1, 0, 0),
    (0, 1, 0),
    (0, -1, 0),
    (0, 0, 1),
    (0, 0, -1),
    (1, 1, 0),
    (-1, -1, 0),
    (1, -1, 0),
    (-1, 1, 0),
    (1, 0, 1),
    (-1, 0, -1),
    (1, 0, -1),
    (-1, 0, 1),
    (0, 1, 1),
    (0, -1, -1),
    (0, 1, -1),
    (0, -1, 1),
)
OPPOSITE = (0, 2, 1, 4, 3, 6, 5, 8, 7, 10, 9, 12, 11, 14, 13, 16, 15, 18, 17)
BASE_RELAX = 0.6
SMAGORINSKY = 0.2
TRACER_RELAX = 0.7

FLOW = 19
MOVING = 26
SOLID, INFLOW, EMISSION = 26, 27, 28
UNITS = 29
SPEED = LATTICE + LATTICE[:7] + ((0, 0, 0),) * 3
TURNED = OPPOSITE + tuple(FLOW + k for k in OPPOSITE[:7])


def split_units(axis, sign):
    along = [u for u in range(UNITS) if SPEED[u][axis] == sign]
    still = [u for u in range(UNITS) if SPEED[u][axis] == 0]
    against = [u for u in range(UNITS) if SPEED[u][axis] == -sign]
    return along, still, against


def wall_pair(axis, sign):
    against = split_units(axis, sign)[2]
    return tuple(next(u for u in against if SPEED[u][2] == step) for step in (-1, 1))


def row_plan(sign):
    plan, offset = [], 0
    for units, depth in zip(split_units(0, sign), (STEPS, STEPS - 1, STEPS - 2)):
        for u in units:
            plan.append((u, STEPS - depth if sign > 0 else 0, depth, offset))
            offset += depth
    return plan, (offset, 1 if sign > 0 else 2), -(-(offset + 1) // ROWS) * ROWS


def pack_rows(read, store, sign, first, height):
    plan, (offset, row), _ = row_plan(sign)
    for u, low, depth, at in plan:
        store(at, depth, read(u, first + low, depth))
    floor, roof = wall_pair(0, sign)
    store(offset, 1, jnp.where(height[:1] == 0, read(floor, first + row, 1), read(roof, first + row, 1)))


def unpack_rows(read, store, sign, first):
    plan, (offset, row), _ = row_plan(sign)
    for u, low, depth, at in plan:
        store(u, first + low, read(at, depth))
    for u in wall_pair(0, sign):
        store(u, first + row, read(offset, 1))


def pack_columns(read, store, sign, lane, nz):
    along, still, against = split_units(1, sign)
    for t, u in enumerate(along):
        store(t, read(u))
    half = LANES // 2
    for t, u in enumerate(still):
        value = read(u)
        if t < 2 * len(against):
            chunk = t % 2
            other = read(against[t // 2])
            if sign > 0:
                value = jnp.where(lane < nz, pltpu.roll(other, half - nz * chunk, 1), value)
            else:
                value = jnp.where(lane >= LANES - nz, pltpu.roll(other, LANES - nz - nz * chunk, 1), value)
        elif t == 2 * len(against):
            floor, roof = wall_pair(1, sign)
            other = jnp.where(lane % nz == 0, read(floor), read(roof))
            if sign > 0:
                value = jnp.where(lane < nz, pltpu.roll(other, LANES - nz, 1), value)
            else:
                value = jnp.where(lane >= LANES - nz, pltpu.roll(other, nz, 1), value)
        store(len(along) + t, value)


def unpack_columns(read, store, sign, lane, nz):
    along, still, against = split_units(1, sign)
    for t, u in enumerate(along):
        store(u, read(t))
    base = len(along)
    for t, u in enumerate(still):
        store(u, read(base + t))
    half = LANES // 2
    for t, u in enumerate(against):
        first, second = read(base + 2 * t), read(base + 2 * t + 1)
        if sign > 0:
            value = jnp.where(lane < LANES - nz, pltpu.roll(first, half, 1), pltpu.roll(second, half + nz, 1))
        else:
            value = jnp.where(lane < nz, pltpu.roll(first, nz, 1), pltpu.roll(second, 2 * nz, 1))
        if u in wall_pair(1, sign):
            walls = read(base + 2 * len(against))
            if sign > 0:
                value = jnp.where(lane < half, pltpu.roll(walls, nz, 1), value)
            else:
                value = jnp.where(lane >= half, pltpu.roll(walls, LANES - nz, 1), value)
        store(u, value)


def relax(h, q, solid, inflow, emission, wind):
    w_rest, w_axis, w_diag = 1.0 / 3.0, 1.0 / 18.0, 1.0 / 36.0
    total = {k: h[k] + h[k + 1] for k in range(1, 19, 2)}
    gap = {k: h[k] - h[k + 1] for k in range(1, 19, 2)}
    xy, xz, yz = total[7] + total[9], total[11] + total[13], total[15] + total[17]
    axes = total[1] + total[3] + total[5]
    density = w_rest * h[0] + w_axis * axes + w_diag * (xy + xz + yz)
    ux = w_axis * gap[1] + w_diag * (gap[7] + gap[9] + gap[11] + gap[13])
    uy = w_axis * gap[3] + w_diag * (gap[7] - gap[9] + gap[15] + gap[17])
    uz = w_axis * gap[5] + w_diag * (gap[11] - gap[13] + gap[15] - gap[17])
    uxx, uyy, uzz = ux * ux, uy * uy, uz * uz
    third = w_rest * density
    pxx = w_axis * total[1] + w_diag * (xy + xz) - third - uxx
    pyy = w_axis * total[3] + w_diag * (xy + yz) - third - uyy
    pzz = w_axis * total[5] + w_diag * (xz + yz) - third - uzz
    pxy = w_diag * (total[7] - total[9]) - ux * uy
    pxz = w_diag * (total[11] - total[13]) - ux * uz
    pyz = w_diag * (total[15] - total[17]) - uy * uz
    cross = pxy * pxy + pxz * pxz + pyz * pyz
    contraction = pxx * pxx + pyy * pyy + pzz * pzz + (cross + cross)
    strength = 18.0 * math.sqrt(2.0) * SMAGORINSKY * SMAGORINSKY
    relax_time = 0.5 * (BASE_RELAX + jnp.sqrt(BASE_RELAX * BASE_RELAX + strength * jnp.sqrt(contraction)))
    rate = 1.0 / relax_time

    keep = 1.0 - 1.0 / TRACER_RELAX
    amount = 0.25 * q[0] + 0.125 * ((q[1] + q[2]) + (q[3] + q[4]) + (q[5] + q[6]))
    source = jnp.where(inflow, 0.0, amount * (1.0 / TRACER_RELAX))
    hold = jnp.where(inflow, 0.0, keep)
    level = source + jnp.where(inflow, 0.0, emission)
    push = 4.0 * source
    traced = [None] * 7
    traced[0] = jnp.where(solid, q[0], hold * q[0] + level)
    for k, speed in ((1, ux), (3, uy), (5, uz)):
        shift = push * speed
        traced[k] = jnp.where(solid, q[k + 1], hold * q[k] + (level + shift))
        traced[k + 1] = jnp.where(solid, q[k], hold * q[k + 1] + (level - shift))

    rate = jnp.where(inflow, 1.0, rate)
    density = jnp.where(inflow, 1.0, density)
    ux, uy, uz = (jnp.where(inflow, w, u) for w, u in zip(wind, (ux, uy, uz)))
    rest = 1.0 - rate
    square = ux * ux + uy * uy + uz * uz
    base = rate * (density - 1.5 * square)
    linear = 3.0 * rate
    quadratic = 4.5 * rate
    relaxed = [None] * 19
    relaxed[0] = jnp.where(solid, h[0], rest * h[0] + base)
    along = {1: ux, 3: uy, 5: uz, 7: ux + uy, 9: ux - uy, 11: ux + uz, 13: ux - uz, 15: uy + uz, 17: uy - uz}
    for k, speed in along.items():
        even = base + quadratic * speed * speed
        odd = linear * speed
        relaxed[k] = jnp.where(solid, h[k + 1], rest * h[k] + (even + odd))
        relaxed[k + 1] = jnp.where(solid, h[k], rest * h[k + 1] + (even - odd))
    return relaxed + traced


def by_side(axis, body, near, far):
    even = lax.axis_index(axis) % 2 == 0
    pl.when(even)(lambda: body(near, far))
    pl.when(jnp.logical_not(even))(lambda: body(far, near))


def lane_index():
    return lax.broadcasted_iota(jnp.int32, (ROWS, LANES), 1)


def wind_tiles(wind):
    return [jnp.broadcast_to(wind[a : a + 1, :], (ROWS, LANES)) for a in range(3)]


def start_all(copies, sems):
    started = [pltpu.make_async_copy(src, dst, sems.at[n]) for n, (src, dst) in enumerate(copies)]
    for copy in started:
        copy.start()
    return started


def relax_own(cells, winds, store, rows):
    populations, tracer, solid, inflow, emission = cells
    h = [populations[k, rows, :] for k in range(FLOW)]
    q = [tracer[k, rows, :] for k in range(7)]
    built, held, emitted = solid[rows, :], inflow[rows, :], emission[rows, :]
    out = relax(h, q, built == 1, held == 1, emitted, winds)
    for u, value in enumerate(out + [built.astype(jnp.float32), held.astype(jnp.float32), emitted]):
        store(u, value)


def load_tiles(arrays, buffers, columns, sems, extra=()):
    copies = list(extra)
    for n, j in enumerate(columns):
        lanes = pl.ds(j * LANES, LANES)
        for array, buffer in zip(arrays, buffers):
            src = array.at[:, :, lanes] if len(array.shape) == 3 else array.at[:, lanes]
            copies.append((src, buffer.at[n]))
    started = start_all(copies, sems)
    count = len(arrays)
    own = [started[len(extra) + n * count : len(extra) + (n + 1) * count] for n in range(len(columns))]
    return started[: len(extra)], own


def first_edges(
    populations, tracer, solid, inflow, wind, emission, one, winds, y_near, y_far,
    wind_in, pop_in, tracer_in, solid_in, inflow_in, emission_in, sems,
):
    extent = populations.shape[1]
    tiles = populations.shape[2] // LANES
    nz = wind.shape[1]
    lane = lane_index()
    buffers = (pop_in, tracer_in, solid_in, inflow_in, emission_in)
    common, own = load_tiles(
        (populations, tracer, solid, inflow, emission), buffers, (tiles - 1, 0), sems, ((wind, wind_in),)
    )
    for copy in common:
        copy.wait()
    winds[...] = jnp.concatenate([wind_in[...]] * (LANES // nz), axis=1)
    wind_values = wind_tiles(winds)
    for n, at in enumerate((tiles, 1)):
        for copy in own[n]:
            copy.wait()
        cells = [b.at[n] for b in buffers]
        for r in range(0, extent, ROWS):
            rows = slice(r, r + ROWS)

            def keep(u, value, at=at, r=r):
                one[u, at, STEPS + r : STEPS + r + ROWS, :] = value

            relax_own(cells, wind_values, keep, rows)

    def pack(up, down):
        for at, sign, target in ((tiles, 1, up), (1, -1, down)):
            for r in range(0, extent, ROWS):
                def send(t, value, target=target, r=r):
                    target[t, r : r + ROWS, :] = value

                pack_columns(
                    lambda u, at=at, r=r: one[u, at, STEPS + r : STEPS + r + ROWS, :], send, sign, lane, nz
                )

    by_side("gy", pack, y_near, y_far)


def first_inner(
    populations, tracer, solid, inflow, emission, winds, _, one, x_near, x_far,
    pop_in, tracer_in, solid_in, inflow_in, emission_in, sems, *, nz,
):
    extent = populations.shape[1]
    tiles = populations.shape[2] // LANES
    height = lane_index() % nz
    buffers = (pop_in, tracer_in, solid_in, inflow_in, emission_in)
    columns = tuple(range(1, tiles - 1))
    _, own = load_tiles((populations, tracer, solid, inflow, emission), buffers, columns, sems)
    wind_values = wind_tiles(winds)

    for n, j in enumerate(columns):
        for copy in own[n]:
            copy.wait()
        for r in range(0, extent, ROWS):
            rows = slice(r, r + ROWS)

            def keep(u, value, j=j, r=r):
                one[u, j + 1, STEPS + r : STEPS + r + ROWS, :] = value

            relax_own([b.at[n] for b in buffers], wind_values, keep, rows)
    by_side("gx", lambda up, down: pack_sides(one, range(1, tiles + 1), up, down, extent, height), x_near, x_far)


def pack_sides(one, columns, up, down, extent, height):
    for at, c in enumerate(columns):
        for sign, target, first in ((1, up, extent), (-1, down, STEPS)):
            def store(offset, depth, value, target=target, at=at):
                target[at, offset : offset + depth, :] = value

            pack_rows(lambda u, low, depth, c=c: one[u, c, low : low + depth, :], store, sign, first, height)


def turn_corner(from_near, from_far, _, one, x_near, x_far, *, nz):
    wide = one.shape[1]
    extent = one.shape[2] - 2 * STEPS
    lane = lane_index()
    height = lane % nz

    def unpack(north, south):
        for sign, source, at in ((1, south, 0), (-1, north, wide - 1)):
            for r in range(0, extent, ROWS):
                def store(u, value, at=at, r=r):
                    one[u, at, STEPS + r : STEPS + r + ROWS, :] = value

                unpack_columns(lambda t, source=source, r=r: source[t, r : r + ROWS, :], store, sign, lane, nz)

    by_side("gy", unpack, from_near, from_far)
    by_side("gx", lambda up, down: pack_sides(one, (0, wide - 1), up, down, extent, height), x_near, x_far)


class Mover:
    def __init__(self, nz):
        lane = lane_index()
        height = lane % nz
        self.nz = nz
        self.from_part = [None] + [lane >= part * nz for part in range(1, LANES // nz)]
        self.floor, self.roof = height == 0, height == nz - 1

    def merge(self, read, columns):
        value = read(columns[0])
        for part in range(1, len(columns)):
            if columns[part] != columns[part - 1]:
                value = jnp.where(self.from_part[part], read(columns[part]), value)
        return value

    def pull(self, read, parts, u):
        step_x, step_y, step_z = SPEED[u]
        value = self.merge(lambda c: read(u, c, step_x), parts[step_y])
        shift = (self.nz * step_y + step_z) % LANES
        if shift:
            value = pltpu.roll(value, shift, 1)
        if step_z:
            own = self.merge(lambda c: read(TURNED[u], c, 0), parts[0])
            value = jnp.where(self.floor if step_z == 1 else self.roof, own, value)
        return value


class Block:
    def __init__(self, one, two, three, four, done, winds, nz):
        self.levels = (None, one, two, three, four)
        self.done = done
        self.tiles = done.shape[1]
        self.extent = done.shape[2]
        self.last = self.tiles + 1
        self.both = self.tiles + 2
        self.count = LANES // nz
        self.mover = Mover(nz)
        self.winds = wind_tiles(winds)
        self.upper = lax.broadcasted_iota(jnp.int32, (ROWS, LANES), 0) < ROWS // 2

    def centre(self, step):
        low, high = STEPS + step, STEPS + self.extent - step
        return list(range(low, high - ROWS, ROWS)) + [high - ROWS]

    def seam(self, step):
        return (step, STEPS + self.extent - step)

    def read(self, level, u, c, place, back=0):
        ref = self.levels[level]
        if isinstance(place, tuple):
            low, high = place[0] - back, place[1] - back - ROWS // 2
            return jnp.where(self.upper, ref[u, c, low : low + ROWS, :], ref[u, c, high : high + ROWS, :])
        return ref[u, c, place - back : place - back + ROWS, :]

    def write(self, ref, u, c, place, value, lift=0):
        if isinstance(place, tuple):
            half = ROWS // 2
            ref[u, c, place[0] - lift : place[0] - lift + half, :] = value[:half]
            ref[u, c, place[1] - lift : place[1] - lift + half, :] = value[half:]
        else:
            ref[u, c, place - lift : place - lift + ROWS, :] = value

    def sources(self, level, c, before, after):
        tiles, last, both, count = self.tiles, self.last, self.both, self.count
        half = count // 2
        if c == both and level < 3:
            return {
                0: [last] * half + [0] * (count - half),
                1: [last] * (half - 1) + [0] * (count - half) + [tiles],
                -1: [1] + [last] * half + [0] * (count - half - 1),
            }
        return {0: [c] * count, 1: [c] * (count - 1) + [before], -1: [after] + [c] * (count - 1)}

    def around(self, level, c, margins):
        if not margins:
            return max(c - 1, 1), min(c + 1, self.tiles)
        if c == self.both:
            return self.tiles, 1
        before = self.both if c == 1 and level > 2 else max(c - 1, 0)
        after = self.both if c == self.tiles and level > 2 else min(c + 1, self.last)
        return before, after

    def pull(self, level, c, place, margins):
        parts = self.sources(level, c, *self.around(level, c, margins))
        return [
            self.mover.pull(lambda v, at, back: self.read(level, v, at, place, back), parts, u) for u in range(MOVING)
        ]

    def relax(self, step, c, place, margins):
        moved = self.pull(step, c, place, margins)
        here = self.sources(1, c, c, c)[0]
        solid, inflow, emission = (
            self.mover.merge(lambda at, u=u: self.read(1, u, at, place), here) for u in (SOLID, INFLOW, EMISSION)
        )
        out = relax(moved[:FLOW], moved[FLOW:], solid == 1.0, inflow == 1.0, emission, self.winds)
        for u in range(MOVING):
            self.write(self.levels[step + 1], u, c, place, out[u])

    def finish(self, c, place, margins):
        for u, value in enumerate(self.pull(STEPS, c, place, margins)):
            self.write(self.done, u, c - 1, place, value, STEPS)

    def steps(self, columns, places, margins):
        for step in range(1, STEPS):
            for c in columns(step):
                for place in places(step):
                    self.relax(step, c, place, margins)

    def inner(self, places):
        self.steps(lambda step: range(1, self.tiles + 1), places, False)
        for c in range(2, self.tiles):
            for place in places(STEPS):
                self.finish(c, place, False)

    def outer(self, places):
        self.steps(
            lambda step: (0, 1, self.tiles, self.last) if step == 1 else (self.both, 1, self.tiles), places, True
        )
        for c in (1, self.tiles):
            for place in places(STEPS):
                self.finish(c, place, True)


def inner_centre(winds, _, one, two, three, four, done, *, nz):
    block = Block(one, two, three, four, done, winds, nz)
    block.inner(block.centre)


def inner_seam(winds, near, far, *refs, nz):
    one, two, three, four, done = refs[5:]
    block = Block(one, two, three, four, done, winds, nz)
    columns = range(1, block.tiles + 1)
    by_side("gx", lambda east, west: fill_rows(one, columns, west, east, block.extent), near, far)
    block.inner(lambda step: [block.seam(step)])


def fill_rows(one, columns, west, east, extent):
    for at, c in enumerate(columns):
        for sign, source, first in ((1, west, 0), (-1, east, STEPS + extent)):
            def fill(u, row, value, c=c):
                one[u, c, row : row + value.shape[0], :] = value

            unpack_rows(
                lambda offset, depth, source=source, at=at: source[at, offset : offset + depth, :], fill, sign, first
            )


def outer_centre(winds, *refs, nz):
    block = Block(*refs[5:], winds, nz)
    block.outer(block.centre)


def outer_seam(winds, near, far, *refs, nz):
    one, two, three, four, done, flow_out, tracer_out, sems = refs[5:]
    block = Block(one, two, three, four, done, winds, nz)
    copies = []

    def write_out(j):
        lanes = pl.ds(j * LANES, LANES)
        for first, number, target in ((0, FLOW, flow_out), (FLOW, 7, tracer_out)):
            copy = pltpu.make_async_copy(
                done.at[pl.ds(first, number), j], target.at[:, :, lanes], sems.at[len(copies)]
            )
            copy.start()
            copies.append(copy)

    for j in range(1, block.tiles - 1):
        write_out(j)
    columns = (0, block.last)
    by_side("gx", lambda east, west: fill_rows(one, columns, west, east, block.extent), near, far)
    block.steps(
        lambda step: (0, 1, block.tiles, block.last) if step == 1 else (block.both, 1, block.tiles),
        lambda step: [block.seam(step)],
        True,
    )
    for c in (1, block.tiles):
        block.finish(c, block.seam(STEPS), True)
        write_out(c - 1)
    for copy in copies:
        copy.wait()


def swapped(shard, axis, start):
    length = lax.axis_size(axis)
    pairs = [((i + start) % length, ((i ^ 1) + start) % length) for i in range(length)]
    return lax.ppermute(shard, axis, pairs)


def local(populations, tracer, solid_mask, inflow, wind_profile, emission):
    extent = populations.shape[1]
    tiles = populations.shape[2] // LANES
    nz = wind_profile.shape[1]
    inner_tiles = tiles - 2
    along, still, _ = split_units(1, 1)
    messages = len(along) + len(still)
    packed = row_plan(1)[2]
    rows = extent + 2 * STEPS
    vm = lambda *shape: pltpu.VMEM(shape, jnp.float32)
    far = pl.BlockSpec(memory_space=pltpu.HBM)
    close = pl.BlockSpec(memory_space=pltpu.VMEM)

    def buffers(number):
        return [
            vm(number, FLOW, extent, LANES),
            vm(number, 7, extent, LANES),
            pltpu.VMEM((number, extent, LANES), jnp.int32),
            pltpu.VMEM((number, extent, LANES), jnp.int32),
            vm(number, extent, LANES),
            pltpu.SemaphoreType.DMA((5 * number + 1,)),
        ]

    def run(body, out_shape, args, far_args=0, out_specs=None, scratch=(), aliases=None):
        specs = [far] * far_args + [close] * (len(args) - far_args)
        args = tuple(
            pltpu.with_memory_space_constraint(a, pltpu.HBM if n < far_args else pltpu.VMEM) for n, a in enumerate(args)
        )
        options = {} if out_specs is None else {"out_specs": out_specs}
        return pl.pallas_call(
            body,
            out_shape=out_shape,
            in_specs=specs,
            scratch_shapes=list(scratch),
            input_output_aliases=aliases or {},
            compiler_params=pltpu.CompilerParams(vmem_limit_bytes=KERNEL_BYTES),
            **options,
        )(*args)

    first = vm(UNITS, tiles + 2, rows, LANES)
    levels = (first, vm(MOVING, tiles + 2, rows, LANES)) + (vm(MOVING, tiles + 3, rows, LANES),) * 2
    levels += (vm(MOVING, tiles, extent, LANES),)
    one, winds, y_near, y_far = run(
        first_edges,
        (first, vm(3, LANES), vm(messages, extent, LANES), vm(messages, extent, LANES)),
        (populations, tracer, solid_mask, inflow, wind_profile, emission),
        far_args=6,
        scratch=[vm(3, nz)] + buffers(2),
    )
    y_near = swapped(y_near, "gy", 0)
    y_far = swapped(y_far, "gy", 1)
    one, x_near, x_far = run(
        lambda *refs: first_inner(*refs, nz=nz),
        (first, vm(tiles, packed, LANES), vm(tiles, packed, LANES)),
        (populations, tracer, solid_mask, inflow, emission, winds, one),
        far_args=5,
        scratch=buffers(inner_tiles),
        aliases={6: 0},
    )
    x_near = swapped(x_near, "gx", 0)
    x_far = swapped(x_far, "gx", 1)
    state = run(lambda *refs: inner_centre(*refs, nz=nz), levels, (winds, one), aliases={1: 0})
    one, corner_near, corner_far = run(
        lambda *refs: turn_corner(*refs, nz=nz),
        (first, vm(2, packed, LANES), vm(2, packed, LANES)),
        (y_near, y_far, state[0]),
        aliases={2: 0},
    )
    corner_near = swapped(corner_near, "gx", 0)
    corner_far = swapped(corner_far, "gx", 1)
    state = run(
        lambda *refs: inner_seam(*refs, nz=nz),
        levels,
        (winds, x_near, x_far, one, *state[1:]),
        aliases={3 + n: n for n in range(5)},
    )
    state = run(lambda *refs: outer_centre(*refs, nz=nz), levels, (winds, *state), aliases={1 + n: n for n in range(5)})
    out = run(
        lambda *refs: outer_seam(*refs, nz=nz),
        levels
        + (
            jax.ShapeDtypeStruct((FLOW, extent, tiles * LANES), jnp.float32),
            jax.ShapeDtypeStruct((7, extent, tiles * LANES), jnp.float32),
        ),
        (winds, corner_near, corner_far, *state),
        out_specs=(close,) * 5 + (far, far),
        scratch=[pltpu.SemaphoreType.DMA((2 * tiles,))],
        aliases={3 + n: n for n in range(5)},
    )
    return out[5], out[6]


def solution(mesh):
    in_specs = (
        P(None, "gx", "gy"),
        P(None, "gx", "gy"),
        P("gx", "gy"),
        P("gx", "gy"),
        P(),
        P("gx", "gy"),
    )
    out_specs = (P(None, "gx", "gy"), P(None, "gx", "gy"))

    return jax.shard_map(local, mesh=mesh, in_specs=in_specs, out_specs=out_specs, check_vma=False)
```

```python
import math

import jax
import jax.numpy as jnp
from jax import lax
from jax.experimental import pallas as pl
from jax.experimental.pallas import tpu as pltpu
from jax.sharding import PartitionSpec as P


STEPS = 4
LANES = 128
KERNEL_BYTES = 16 * 2**20
ROWS = 8

LATTICE = (
    (0, 0, 0),
    (1, 0, 0),
    (-1, 0, 0),
    (0, 1, 0),
    (0, -1, 0),
    (0, 0, 1),
    (0, 0, -1),
    (1, 1, 0),
    (-1, -1, 0),
    (1, -1, 0),
    (-1, 1, 0),
    (1, 0, 1),
    (-1, 0, -1),
    (1, 0, -1),
    (-1, 0, 1),
    (0, 1, 1),
    (0, -1, -1),
    (0, 1, -1),
    (0, -1, 1),
)
OPPOSITE = (0, 2, 1, 4, 3, 6, 5, 8, 7, 10, 9, 12, 11, 14, 13, 16, 15, 18, 17)
BASE_RELAX = 0.6
SMAGORINSKY = 0.2
TRACER_RELAX = 0.7

FLOW = 19
MOVING = 26
SOLID, INFLOW, EMISSION = 26, 27, 28
UNITS = 29
SPEED = LATTICE + LATTICE[:7] + ((0, 0, 0),) * 3
TURNED = OPPOSITE + tuple(FLOW + k for k in OPPOSITE[:7])


def split_units(axis, sign):
    along = [u for u in range(UNITS) if SPEED[u][axis] == sign]
    still = [u for u in range(UNITS) if SPEED[u][axis] == 0]
    against = [u for u in range(UNITS) if SPEED[u][axis] == -sign]
    return along, still, against


def wall_pair(axis, sign):
    against = split_units(axis, sign)[2]
    return tuple(next(u for u in against if SPEED[u][2] == step) for step in (-1, 1))


def row_plan(sign):
    plan, offset = [], 0
    for units, depth in zip(split_units(0, sign), (STEPS, STEPS - 1, STEPS - 2)):
        for u in units:
            plan.append((u, STEPS - depth if sign > 0 else 0, depth, offset))
            offset += depth
    return plan, (offset, 1 if sign > 0 else 2), -(-(offset + 1) // ROWS) * ROWS


def pack_rows(read, store, sign, first, height):
    plan, (offset, row), _ = row_plan(sign)
    for u, low, depth, at in plan:
        store(at, depth, read(u, first + low, depth))
    floor, roof = wall_pair(0, sign)
    store(offset, 1, jnp.where(height[:1] == 0, read(floor, first + row, 1), read(roof, first + row, 1)))


def unpack_rows(read, store, sign, first):
    plan, (offset, row), _ = row_plan(sign)
    for u, low, depth, at in plan:
        store(u, first + low, read(at, depth))
    for u in wall_pair(0, sign):
        store(u, first + row, read(offset, 1))


def message_plan(sign):
    along, still, against = split_units(1, sign)
    riders = [(u, chunk) for u in against for chunk in range(2)] + [(None, 0)]
    carried = []
    for unit in still:
        fit = next((r for r in riders if (0 if r[0] is None else SPEED[r[0]][0]) == SPEED[unit][0]), None)
        carried.append(fit)
        if fit is not None:
            riders.remove(fit)
    return along, still, carried


def pack_columns(read, store, sign, lane, nz):
    along, still, carried = message_plan(sign)
    for t, u in enumerate(along):
        store(t, read(u))
    half = LANES // 2
    for t, (u, rider) in enumerate(zip(still, carried)):
        value = read(u)
        if rider is not None:
            unit, chunk = rider
            if unit is None:
                floor, roof = wall_pair(1, sign)
                other = jnp.where(lane % nz == 0, read(floor), read(roof))
                shift = LANES - nz if sign > 0 else nz
            else:
                other = read(unit)
                shift = half - nz * chunk if sign > 0 else LANES - nz - nz * chunk
            spare = lane < nz if sign > 0 else lane >= LANES - nz
            value = jnp.where(spare, pltpu.roll(other, shift, 1), value)
        store(len(along) + t, value)


def unpack_columns(read, store, sign, lane, nz):
    along, still, carried = message_plan(sign)
    for t, u in enumerate(along):
        store(u, read(t))
    base = len(along)
    for t, u in enumerate(still):
        store(u, read(base + t))
    half = LANES // 2
    for u in split_units(1, sign)[2]:
        first, second = (read(base + carried.index((u, chunk))) for chunk in range(2))
        if sign > 0:
            value = jnp.where(lane < LANES - nz, pltpu.roll(first, half, 1), pltpu.roll(second, half + nz, 1))
        else:
            value = jnp.where(lane < nz, pltpu.roll(first, nz, 1), pltpu.roll(second, 2 * nz, 1))
        if u in wall_pair(1, sign):
            walls = read(base + carried.index((None, 0)))
            if sign > 0:
                value = jnp.where(lane < half, pltpu.roll(walls, nz, 1), value)
            else:
                value = jnp.where(lane >= half, pltpu.roll(walls, LANES - nz, 1), value)
        store(u, value)


def corner_plan(sign, sign_y):
    along, still, _ = message_plan(sign_y)
    units = list(along) + list(still)
    plan, offset = [], 0
    for t, u in enumerate(units):
        depth = STEPS - 1 + sign * SPEED[u][0]
        plan.append((t, STEPS - depth if sign > 0 else 0, depth, offset))
        offset += depth
    walls = tuple(units.index(u) for u in wall_pair(0, sign))
    return plan, (offset, 1 if sign > 0 else 2), walls, -(-(offset + 1) // ROWS) * ROWS


def relax(h, q, solid, inflow, emission, wind):
    w_rest, w_axis, w_diag = 1.0 / 3.0, 1.0 / 18.0, 1.0 / 36.0
    total = {k: h[k] + h[k + 1] for k in range(1, 19, 2)}
    gap = {k: h[k] - h[k + 1] for k in range(1, 19, 2)}
    xy, xz, yz = total[7] + total[9], total[11] + total[13], total[15] + total[17]
    axes = total[1] + total[3] + total[5]
    density = w_rest * h[0] + w_axis * axes + w_diag * (xy + xz + yz)
    ux = w_axis * gap[1] + w_diag * (gap[7] + gap[9] + gap[11] + gap[13])
    uy = w_axis * gap[3] + w_diag * (gap[7] - gap[9] + gap[15] + gap[17])
    uz = w_axis * gap[5] + w_diag * (gap[11] - gap[13] + gap[15] - gap[17])
    uxx, uyy, uzz = ux * ux, uy * uy, uz * uz
    third = w_rest * density
    pxx = w_axis * total[1] + w_diag * (xy + xz) - third - uxx
    pyy = w_axis * total[3] + w_diag * (xy + yz) - third - uyy
    pzz = w_axis * total[5] + w_diag * (xz + yz) - third - uzz
    pxy = w_diag * (total[7] - total[9]) - ux * uy
    pxz = w_diag * (total[11] - total[13]) - ux * uz
    pyz = w_diag * (total[15] - total[17]) - uy * uz
    cross = pxy * pxy + pxz * pxz + pyz * pyz
    contraction = pxx * pxx + pyy * pyy + pzz * pzz + (cross + cross)
    strength = 18.0 * math.sqrt(2.0) * SMAGORINSKY * SMAGORINSKY
    relax_time = 0.5 * (BASE_RELAX + jnp.sqrt(BASE_RELAX * BASE_RELAX + strength * jnp.sqrt(contraction)))
    rate = 1.0 / relax_time

    keep = 1.0 - 1.0 / TRACER_RELAX
    amount = 0.25 * q[0] + 0.125 * ((q[1] + q[2]) + (q[3] + q[4]) + (q[5] + q[6]))
    source = jnp.where(inflow, 0.0, amount * (1.0 / TRACER_RELAX))
    hold = jnp.where(inflow, 0.0, keep)
    level = source + jnp.where(inflow, 0.0, emission)
    push = 4.0 * source
    traced = [None] * 7
    traced[0] = jnp.where(solid, q[0], hold * q[0] + level)
    for k, speed in ((1, ux), (3, uy), (5, uz)):
        shift = push * speed
        traced[k] = jnp.where(solid, q[k + 1], hold * q[k] + (level + shift))
        traced[k + 1] = jnp.where(solid, q[k], hold * q[k + 1] + (level - shift))

    rate = jnp.where(inflow, 1.0, rate)
    density = jnp.where(inflow, 1.0, density)
    ux, uy, uz = (jnp.where(inflow, w, u) for w, u in zip(wind, (ux, uy, uz)))
    rest = 1.0 - rate
    square = ux * ux + uy * uy + uz * uz
    base = rate * (density - 1.5 * square)
    linear = 3.0 * rate
    quadratic = 4.5 * rate
    relaxed = [None] * 19
    relaxed[0] = jnp.where(solid, h[0], rest * h[0] + base)
    along = {1: ux, 3: uy, 5: uz, 7: ux + uy, 9: ux - uy, 11: ux + uz, 13: ux - uz, 15: uy + uz, 17: uy - uz}
    for k, speed in along.items():
        even = base + quadratic * speed * speed
        odd = linear * speed
        relaxed[k] = jnp.where(solid, h[k + 1], rest * h[k] + (even + odd))
        relaxed[k + 1] = jnp.where(solid, h[k], rest * h[k + 1] + (even - odd))
    return relaxed + traced


def by_side(axis, body, near, far):
    even = lax.axis_index(axis) % 2 == 0
    pl.when(even)(lambda: body(near, far))
    pl.when(jnp.logical_not(even))(lambda: body(far, near))


def lane_index():
    return lax.broadcasted_iota(jnp.int32, (ROWS, LANES), 1)


def wind_tiles(wind):
    return [jnp.broadcast_to(wind[a : a + 1, :], (ROWS, LANES)) for a in range(3)]


def start_all(copies, sems):
    started = [pltpu.make_async_copy(src, dst, sems.at[n]) for n, (src, dst) in enumerate(copies)]
    for copy in started:
        copy.start()
    return started


def relax_own(cells, winds, store, rows):
    populations, tracer, solid, inflow, emission = cells
    h = [populations[k, rows, :] for k in range(FLOW)]
    q = [tracer[k, rows, :] for k in range(7)]
    built, held, emitted = solid[rows, :], inflow[rows, :], emission[rows, :]
    out = relax(h, q, built == 1, held == 1, emitted, winds)
    for u, value in enumerate(out + [built.astype(jnp.float32), held.astype(jnp.float32), emitted]):
        store(u, value)


def load_tiles(arrays, buffers, columns, sems, extra=()):
    copies = list(extra)
    for n, j in enumerate(columns):
        lanes = pl.ds(j * LANES, LANES)
        for array, buffer in zip(arrays, buffers):
            src = array.at[:, :, lanes] if len(array.shape) == 3 else array.at[:, lanes]
            copies.append((src, buffer.at[n]))
    started = start_all(copies, sems)
    count = len(arrays)
    own = [started[len(extra) + n * count : len(extra) + (n + 1) * count] for n in range(len(columns))]
    return started[: len(extra)], own


def first_edges(
    populations, tracer, solid, inflow, wind, emission, one, winds, y_near, y_far,
    wind_in, pop_in, tracer_in, solid_in, inflow_in, emission_in, sems,
):
    extent = populations.shape[1]
    tiles = populations.shape[2] // LANES
    nz = wind.shape[1]
    lane = lane_index()
    buffers = (pop_in, tracer_in, solid_in, inflow_in, emission_in)
    common, own = load_tiles(
        (populations, tracer, solid, inflow, emission), buffers, (tiles - 1, 0), sems, ((wind, wind_in),)
    )
    for copy in common:
        copy.wait()
    winds[...] = jnp.concatenate([wind_in[...]] * (LANES // nz), axis=1)
    wind_values = wind_tiles(winds)
    for n, at in enumerate((tiles, 1)):
        for copy in own[n]:
            copy.wait()
        cells = [b.at[n] for b in buffers]
        for r in range(0, extent, ROWS):
            rows = slice(r, r + ROWS)

            def keep(u, value, at=at, r=r):
                one[u, at, STEPS + r : STEPS + r + ROWS, :] = value

            relax_own(cells, wind_values, keep, rows)

    def pack(up, down):
        for at, sign, target in ((tiles, 1, up), (1, -1, down)):
            for r in range(0, extent, ROWS):
                def send(t, value, target=target, r=r):
                    target[t, r : r + ROWS, :] = value

                pack_columns(
                    lambda u, at=at, r=r: one[u, at, STEPS + r : STEPS + r + ROWS, :], send, sign, lane, nz
                )

    by_side("gy", pack, y_near, y_far)


def first_inner(
    populations, tracer, solid, inflow, emission, winds, _, one, x_near, x_far,
    pop_in, tracer_in, solid_in, inflow_in, emission_in, sems, *, nz,
):
    extent = populations.shape[1]
    tiles = populations.shape[2] // LANES
    height = lane_index() % nz
    buffers = (pop_in, tracer_in, solid_in, inflow_in, emission_in)
    columns = tuple(range(1, tiles - 1))
    _, own = load_tiles((populations, tracer, solid, inflow, emission), buffers, columns, sems)
    wind_values = wind_tiles(winds)

    for n, j in enumerate(columns):
        for copy in own[n]:
            copy.wait()
        for r in range(0, extent, ROWS):
            rows = slice(r, r + ROWS)

            def keep(u, value, j=j, r=r):
                one[u, j + 1, STEPS + r : STEPS + r + ROWS, :] = value

            relax_own([b.at[n] for b in buffers], wind_values, keep, rows)
    by_side("gx", lambda up, down: pack_sides(one, range(1, tiles + 1), up, down, extent, height), x_near, x_far)


def pack_sides(one, columns, up, down, extent, height):
    for at, c in enumerate(columns):
        for sign, target, first in ((1, up, extent), (-1, down, STEPS)):
            def store(offset, depth, value, target=target, at=at):
                target[at, offset : offset + depth, :] = value

            pack_rows(lambda u, low, depth, c=c: one[u, c, low : low + depth, :], store, sign, first, height)


def turn_corner(y_near, y_far, x_near, x_far, *, nz):
    extent = y_near.shape[1]
    height = lane_index() % nz

    def pack(sources, targets):
        for side, (sign_y, source) in enumerate(zip((1, -1), sources)):
            for sign, target, first in zip((1, -1), targets, (extent - STEPS, 0)):
                plan, (offset, row), (floor, roof), _ = corner_plan(sign, sign_y)
                for t, low, depth, at in plan:
                    target[side, at : at + depth, :] = source[t, first + low : first + low + depth, :]
                at = slice(first + row, first + row + 1)
                target[side, offset : offset + 1, :] = jnp.where(
                    height[:1] == 0, source[floor, at, :], source[roof, at, :]
                )

    by_side(
        "gy",
        lambda north, south: by_side("gx", lambda up, down: pack((south, north), (up, down)), x_near, x_far),
        y_near,
        y_far,
    )


def take_corners(one, near, far, stage, nz):
    wide, extent = one.shape[1], one.shape[2] - 2 * STEPS
    lane = lane_index()

    def lay(east, west):
        for side, sign_y in enumerate((1, -1)):
            for sign, source, first in ((1, west, 0), (-1, east, STEPS)):
                plan, (offset, row), walls, _ = corner_plan(sign, sign_y)
                for t, low, depth, at in plan:
                    stage[side, t, first + low : first + low + depth, :] = source[side, at : at + depth, :]
                for t in walls:
                    stage[side, t, first + row : first + row + 1, :] = source[side, offset : offset + 1, :]

    by_side("gx", lay, near, far)
    for side, (sign_y, c) in enumerate(((1, 0), (-1, wide - 1))):
        def store(u, value, c=c):
            one[u, c, :STEPS, :] = value[:STEPS]
            one[u, c, STEPS + extent :, :] = value[STEPS:]

        unpack_columns(lambda t, side=side: stage[side, t, :, :], store, sign_y, lane, nz)


class Mover:
    def __init__(self, nz):
        lane = lane_index()
        height = lane % nz
        self.nz = nz
        self.from_part = [None] + [lane >= part * nz for part in range(1, LANES // nz)]
        self.floor, self.roof = height == 0, height == nz - 1

    def merge(self, read, columns):
        value = read(columns[0])
        for part in range(1, len(columns)):
            if columns[part] != columns[part - 1]:
                value = jnp.where(self.from_part[part], read(columns[part]), value)
        return value

    def pull(self, read, parts, u):
        step_x, step_y, step_z = SPEED[u]
        value = self.merge(lambda c: read(u, c, step_x), parts[step_y])
        shift = (self.nz * step_y + step_z) % LANES
        if shift:
            value = pltpu.roll(value, shift, 1)
        if step_z:
            own = self.merge(lambda c: read(TURNED[u], c, 0), parts[0])
            value = jnp.where(self.floor if step_z == 1 else self.roof, own, value)
        return value


class Block:
    def __init__(self, one, two, three, four, done, winds, nz):
        self.levels = (None, one, two, three, four)
        self.done = done
        self.tiles = done.shape[1]
        self.extent = done.shape[2]
        self.last = self.tiles + 1
        self.both = self.tiles + 2
        self.count = LANES // nz
        self.mover = Mover(nz)
        self.winds = wind_tiles(winds)
        self.upper = lax.broadcasted_iota(jnp.int32, (ROWS, LANES), 0) < ROWS // 2

    def centre(self, step):
        low, high = STEPS + step, STEPS + self.extent - step
        return list(range(low, high - ROWS, ROWS)) + [high - ROWS]

    def seam(self, step):
        return (step, STEPS + self.extent - step)

    def read(self, level, u, c, place, back=0):
        ref = self.levels[level]
        if isinstance(place, tuple):
            low, high = place[0] - back, place[1] - back - ROWS // 2
            return jnp.where(self.upper, ref[u, c, low : low + ROWS, :], ref[u, c, high : high + ROWS, :])
        return ref[u, c, place - back : place - back + ROWS, :]

    def write(self, ref, u, c, place, value, lift=0):
        if isinstance(place, tuple):
            half = ROWS // 2
            ref[u, c, place[0] - lift : place[0] - lift + half, :] = value[:half]
            ref[u, c, place[1] - lift : place[1] - lift + half, :] = value[half:]
        else:
            ref[u, c, place - lift : place - lift + ROWS, :] = value

    def sources(self, level, c, before, after):
        tiles, last, both, count = self.tiles, self.last, self.both, self.count
        half = count // 2
        if c == both and level < 3:
            return {
                0: [last] * half + [0] * (count - half),
                1: [last] * (half - 1) + [0] * (count - half) + [tiles],
                -1: [1] + [last] * half + [0] * (count - half - 1),
            }
        return {0: [c] * count, 1: [c] * (count - 1) + [before], -1: [after] + [c] * (count - 1)}

    def around(self, level, c, margins):
        if not margins:
            return max(c - 1, 1), min(c + 1, self.tiles)
        if c == self.both:
            return self.tiles, 1
        before = self.both if c == 1 and level > 2 else max(c - 1, 0)
        after = self.both if c == self.tiles and level > 2 else min(c + 1, self.last)
        return before, after

    def pull(self, level, c, place, margins):
        parts = self.sources(level, c, *self.around(level, c, margins))
        return [
            self.mover.pull(lambda v, at, back: self.read(level, v, at, place, back), parts, u) for u in range(MOVING)
        ]

    def relax(self, step, c, place, margins):
        moved = self.pull(step, c, place, margins)
        here = self.sources(1, c, c, c)[0]
        solid, inflow, emission = (
            self.mover.merge(lambda at, u=u: self.read(1, u, at, place), here) for u in (SOLID, INFLOW, EMISSION)
        )
        out = relax(moved[:FLOW], moved[FLOW:], solid == 1.0, inflow == 1.0, emission, self.winds)
        for u in range(MOVING):
            self.write(self.levels[step + 1], u, c, place, out[u])

    def finish(self, c, place, margins):
        for u, value in enumerate(self.pull(STEPS, c, place, margins)):
            self.write(self.done, u, c - 1, place, value, STEPS)

    def steps(self, columns, places, margins):
        for step in range(1, STEPS):
            for c in columns(step):
                for place in places(step):
                    self.relax(step, c, place, margins)

    def inner(self, places):
        self.steps(lambda step: range(1, self.tiles + 1), places, False)
        for c in range(2, self.tiles):
            for place in places(STEPS):
                self.finish(c, place, False)

    def outer(self, places):
        self.steps(
            lambda step: (0, 1, self.tiles, self.last) if step == 1 else (self.both, 1, self.tiles), places, True
        )
        for c in (1, self.tiles):
            for place in places(STEPS):
                self.finish(c, place, True)


def inner_centre(winds, _, one, two, three, four, done, *, nz):
    block = Block(one, two, three, four, done, winds, nz)
    block.inner(block.centre)


def inner_seam(winds, near, far, *refs, nz):
    one, two, three, four, done = refs[5:]
    block = Block(one, two, three, four, done, winds, nz)
    columns = range(1, block.tiles + 1)
    by_side("gx", lambda east, west: fill_rows(one, columns, west, east, block.extent), near, far)
    block.inner(lambda step: [block.seam(step)])


def fill_rows(one, columns, west, east, extent):
    for at, c in enumerate(columns):
        for sign, source, first in ((1, west, 0), (-1, east, STEPS + extent)):
            def fill(u, row, value, c=c):
                one[u, c, row : row + value.shape[0], :] = value

            unpack_rows(
                lambda offset, depth, source=source, at=at: source[at, offset : offset + depth, :], fill, sign, first
            )


def outer_centre(winds, near, far, *refs, nz):
    one = refs[5]
    block = Block(*refs[5:], winds, nz)
    lane = lane_index()

    def unpack(north, south):
        for sign, source, c in ((1, south, 0), (-1, north, block.last)):
            for r in range(0, block.extent, ROWS):
                def store(u, value, c=c, r=r):
                    one[u, c, STEPS + r : STEPS + r + ROWS, :] = value

                unpack_columns(lambda t, source=source, r=r: source[t, r : r + ROWS, :], store, sign, lane, nz)

    by_side("gy", unpack, near, far)
    block.outer(block.centre)


def outer_seam(winds, near, far, *refs, nz):
    one, two, three, four, done, flow_out, tracer_out, stage, sems = refs[5:]
    block = Block(one, two, three, four, done, winds, nz)
    copies = []

    def write_out(j):
        lanes = pl.ds(j * LANES, LANES)
        for first, number, target in ((0, FLOW, flow_out), (FLOW, 7, tracer_out)):
            copy = pltpu.make_async_copy(
                done.at[pl.ds(first, number), j], target.at[:, :, lanes], sems.at[len(copies)]
            )
            copy.start()
            copies.append(copy)

    for j in range(1, block.tiles - 1):
        write_out(j)
    take_corners(one, near, far, stage, nz)
    block.steps(
        lambda step: (0, 1, block.tiles, block.last) if step == 1 else (block.both, 1, block.tiles),
        lambda step: [block.seam(step)],
        True,
    )
    for c in (1, block.tiles):
        block.finish(c, block.seam(STEPS), True)
        write_out(c - 1)
    for copy in copies:
        copy.wait()


def swapped(shard, axis, start):
    length = lax.axis_size(axis)
    pairs = [((i + start) % length, ((i ^ 1) + start) % length) for i in range(length)]
    return lax.ppermute(shard, axis, pairs)


def local(populations, tracer, solid_mask, inflow, wind_profile, emission):
    extent = populations.shape[1]
    tiles = populations.shape[2] // LANES
    nz = wind_profile.shape[1]
    inner_tiles = tiles - 2
    along, still, _ = split_units(1, 1)
    messages = len(along) + len(still)
    packed = row_plan(1)[2]
    rows = extent + 2 * STEPS
    vm = lambda *shape: pltpu.VMEM(shape, jnp.float32)
    far = pl.BlockSpec(memory_space=pltpu.HBM)
    close = pl.BlockSpec(memory_space=pltpu.VMEM)

    def buffers(number):
        return [
            vm(number, FLOW, extent, LANES),
            vm(number, 7, extent, LANES),
            pltpu.VMEM((number, extent, LANES), jnp.int32),
            pltpu.VMEM((number, extent, LANES), jnp.int32),
            vm(number, extent, LANES),
            pltpu.SemaphoreType.DMA((5 * number + 1,)),
        ]

    def run(body, out_shape, args, far_args=0, out_specs=None, scratch=(), aliases=None):
        specs = [far] * far_args + [close] * (len(args) - far_args)
        args = tuple(
            pltpu.with_memory_space_constraint(a, pltpu.HBM if n < far_args else pltpu.VMEM) for n, a in enumerate(args)
        )
        options = {} if out_specs is None else {"out_specs": out_specs}
        return pl.pallas_call(
            body,
            out_shape=out_shape,
            in_specs=specs,
            scratch_shapes=list(scratch),
            input_output_aliases=aliases or {},
            compiler_params=pltpu.CompilerParams(vmem_limit_bytes=KERNEL_BYTES),
            **options,
        )(*args)

    first = vm(UNITS, tiles + 2, rows, LANES)
    levels = (first, vm(MOVING, tiles + 2, rows, LANES)) + (vm(MOVING, tiles + 3, rows, LANES),) * 2
    levels += (vm(MOVING, tiles, extent, LANES),)
    one, winds, y_near, y_far = run(
        first_edges,
        (first, vm(3, LANES), vm(messages, extent, LANES), vm(messages, extent, LANES)),
        (populations, tracer, solid_mask, inflow, wind_profile, emission),
        far_args=6,
        scratch=[vm(3, nz)] + buffers(2),
    )
    y_near = swapped(y_near, "gy", 0)
    y_far = swapped(y_far, "gy", 1)
    one, x_near, x_far = run(
        lambda *refs: first_inner(*refs, nz=nz),
        (first, vm(tiles, packed, LANES), vm(tiles, packed, LANES)),
        (populations, tracer, solid_mask, inflow, emission, winds, one),
        far_args=5,
        scratch=buffers(inner_tiles),
        aliases={6: 0},
    )
    x_near = swapped(x_near, "gx", 0)
    x_far = swapped(x_far, "gx", 1)
    state = run(lambda *refs: inner_centre(*refs, nz=nz), levels, (winds, one), aliases={1: 0})
    turned = corner_plan(1, 1)[3]
    corner_near, corner_far = run(
        lambda *refs: turn_corner(*refs, nz=nz), (vm(2, turned, LANES), vm(2, turned, LANES)), (y_near, y_far)
    )
    corner_near = swapped(corner_near, "gx", 0)
    corner_far = swapped(corner_far, "gx", 1)
    state = run(
        lambda *refs: outer_centre(*refs, nz=nz),
        levels,
        (winds, y_near, y_far, *state),
        aliases={3 + n: n for n in range(5)},
    )
    state = run(
        lambda *refs: inner_seam(*refs, nz=nz),
        levels,
        (winds, x_near, x_far, *state),
        aliases={3 + n: n for n in range(5)},
    )
    out = run(
        lambda *refs: outer_seam(*refs, nz=nz),
        levels
        + (
            jax.ShapeDtypeStruct((FLOW, extent, tiles * LANES), jnp.float32),
            jax.ShapeDtypeStruct((7, extent, tiles * LANES), jnp.float32),
        ),
        (winds, corner_near, corner_far, *state),
        out_specs=(close,) * 5 + (far, far),
        scratch=[vm(2, messages, ROWS, LANES), pltpu.SemaphoreType.DMA((2 * tiles,))],
        aliases={3 + n: n for n in range(5)},
    )
    return out[5], out[6]


def solution(mesh):
    in_specs = (
        P(None, "gx", "gy"),
        P(None, "gx", "gy"),
        P("gx", "gy"),
        P("gx", "gy"),
        P(),
        P("gx", "gy"),
    )
    out_specs = (P(None, "gx", "gy"), P(None, "gx", "gy"))

    return jax.shard_map(local, mesh=mesh, in_specs=in_specs, out_specs=out_specs, check_vma=False)
```

```python
import math

import jax
import jax.numpy as jnp
from jax import lax
from jax.experimental import pallas as pl
from jax.experimental.pallas import tpu as pltpu
from jax.sharding import PartitionSpec as P


STEPS = 4
LANES = 128
KERNEL_BYTES = 16 * 2**20
ROWS = 8

LATTICE = (
    (0, 0, 0),
    (1, 0, 0),
    (-1, 0, 0),
    (0, 1, 0),
    (0, -1, 0),
    (0, 0, 1),
    (0, 0, -1),
    (1, 1, 0),
    (-1, -1, 0),
    (1, -1, 0),
    (-1, 1, 0),
    (1, 0, 1),
    (-1, 0, -1),
    (1, 0, -1),
    (-1, 0, 1),
    (0, 1, 1),
    (0, -1, -1),
    (0, 1, -1),
    (0, -1, 1),
)
OPPOSITE = (0, 2, 1, 4, 3, 6, 5, 8, 7, 10, 9, 12, 11, 14, 13, 16, 15, 18, 17)
BASE_RELAX = 0.6
SMAGORINSKY = 0.2
TRACER_RELAX = 0.7

FLOW = 19
MOVING = 26
SOLID, INFLOW, EMISSION = 26, 27, 28
UNITS = 29
SPEED = LATTICE + LATTICE[:7] + ((0, 0, 0),) * 3
TURNED = OPPOSITE + tuple(FLOW + k for k in OPPOSITE[:7])


def split_units(axis, sign):
    along = [u for u in range(UNITS) if SPEED[u][axis] == sign]
    still = [u for u in range(UNITS) if SPEED[u][axis] == 0]
    against = [u for u in range(UNITS) if SPEED[u][axis] == -sign]
    return along, still, against


def wall_pair(axis, sign):
    against = split_units(axis, sign)[2]
    return tuple(next(u for u in against if SPEED[u][2] == step) for step in (-1, 1))


def row_plan(sign):
    plan, offset = [], 0
    for units, depth in zip(split_units(0, sign), (STEPS, STEPS - 1, STEPS - 2)):
        for u in units:
            plan.append((u, STEPS - depth if sign > 0 else 0, depth, offset))
            offset += depth
    return plan, (offset, 1 if sign > 0 else 2), -(-(offset + 1) // ROWS) * ROWS


def pack_rows(read, store, sign, first, height):
    plan, (offset, row), _ = row_plan(sign)
    for u, low, depth, at in plan:
        store(at, depth, read(u, first + low, depth))
    floor, roof = wall_pair(0, sign)
    store(offset, 1, jnp.where(height[:1] == 0, read(floor, first + row, 1), read(roof, first + row, 1)))


def unpack_rows(read, store, sign, first):
    plan, (offset, row), _ = row_plan(sign)
    for u, low, depth, at in plan:
        store(u, first + low, read(at, depth))
    for u in wall_pair(0, sign):
        store(u, first + row, read(offset, 1))


def message_plan(sign):
    along, still, against = split_units(1, sign)
    riders = [(u, chunk) for u in against for chunk in range(2)] + [(None, 0)]
    carried = []
    for unit in still:
        fit = next((r for r in riders if (0 if r[0] is None else SPEED[r[0]][0]) == SPEED[unit][0]), None)
        carried.append(fit)
        if fit is not None:
            riders.remove(fit)
    return along, still, carried


def pack_columns(read, store, sign, lane, nz):
    along, still, carried = message_plan(sign)
    for t, u in enumerate(along):
        store(t, read(u))
    half = LANES // 2
    for t, (u, rider) in enumerate(zip(still, carried)):
        value = read(u)
        if rider is not None:
            unit, chunk = rider
            if unit is None:
                floor, roof = wall_pair(1, sign)
                other = jnp.where(lane % nz == 0, read(floor), read(roof))
                shift = LANES - nz if sign > 0 else nz
            else:
                other = read(unit)
                shift = half - nz * chunk if sign > 0 else LANES - nz - nz * chunk
            spare = lane < nz if sign > 0 else lane >= LANES - nz
            value = jnp.where(spare, pltpu.roll(other, shift, 1), value)
        store(len(along) + t, value)


def unpack_columns(read, store, sign, lane, nz):
    along, still, carried = message_plan(sign)
    for t, u in enumerate(along):
        store(u, read(t))
    base = len(along)
    for t, u in enumerate(still):
        store(u, read(base + t))
    half = LANES // 2
    for u in split_units(1, sign)[2]:
        first, second = (read(base + carried.index((u, chunk))) for chunk in range(2))
        if sign > 0:
            value = jnp.where(lane < LANES - nz, pltpu.roll(first, half, 1), pltpu.roll(second, half + nz, 1))
        else:
            value = jnp.where(lane < nz, pltpu.roll(first, nz, 1), pltpu.roll(second, 2 * nz, 1))
        if u in wall_pair(1, sign):
            walls = read(base + carried.index((None, 0)))
            if sign > 0:
                value = jnp.where(lane < half, pltpu.roll(walls, nz, 1), value)
            else:
                value = jnp.where(lane >= half, pltpu.roll(walls, LANES - nz, 1), value)
        store(u, value)


def corner_plan(sign, sign_y):
    along, still, _ = message_plan(sign_y)
    units = list(along) + list(still)
    plan, offset = [], 0
    for t, u in enumerate(units):
        depth = STEPS - 1 + sign * SPEED[u][0]
        plan.append((t, STEPS - depth if sign > 0 else 0, depth, offset))
        offset += depth
    walls = tuple(units.index(u) for u in wall_pair(0, sign))
    return plan, (offset, 1 if sign > 0 else 2), walls, -(-(offset + 1) // ROWS) * ROWS


def relax(h, q, solid, inflow, emission, wind):
    w_rest, w_axis, w_diag = 1.0 / 3.0, 1.0 / 18.0, 1.0 / 36.0
    total = {k: h[k] + h[k + 1] for k in range(1, 19, 2)}
    gap = {k: h[k] - h[k + 1] for k in range(1, 19, 2)}
    xy, xz, yz = total[7] + total[9], total[11] + total[13], total[15] + total[17]
    axes = total[1] + total[3] + total[5]
    density = w_rest * h[0] + w_axis * axes + w_diag * (xy + xz + yz)
    ux = w_axis * gap[1] + w_diag * (gap[7] + gap[9] + gap[11] + gap[13])
    uy = w_axis * gap[3] + w_diag * (gap[7] - gap[9] + gap[15] + gap[17])
    uz = w_axis * gap[5] + w_diag * (gap[11] - gap[13] + gap[15] - gap[17])
    uxx, uyy, uzz = ux * ux, uy * uy, uz * uz
    third = w_rest * density
    pxx = w_axis * total[1] + w_diag * (xy + xz) - third - uxx
    pyy = w_axis * total[3] + w_diag * (xy + yz) - third - uyy
    pzz = w_axis * total[5] + w_diag * (xz + yz) - third - uzz
    pxy = w_diag * (total[7] - total[9]) - ux * uy
    pxz = w_diag * (total[11] - total[13]) - ux * uz
    pyz = w_diag * (total[15] - total[17]) - uy * uz
    cross = pxy * pxy + pxz * pxz + pyz * pyz
    contraction = pxx * pxx + pyy * pyy + pzz * pzz + (cross + cross)
    strength = 18.0 * math.sqrt(2.0) * SMAGORINSKY * SMAGORINSKY
    relax_time = 0.5 * (BASE_RELAX + jnp.sqrt(BASE_RELAX * BASE_RELAX + strength * jnp.sqrt(contraction)))
    rate = 1.0 / relax_time

    keep = 1.0 - 1.0 / TRACER_RELAX
    amount = 0.25 * q[0] + 0.125 * ((q[1] + q[2]) + (q[3] + q[4]) + (q[5] + q[6]))
    source = jnp.where(inflow, 0.0, amount * (1.0 / TRACER_RELAX))
    hold = jnp.where(inflow, 0.0, keep)
    level = source + jnp.where(inflow, 0.0, emission)
    push = 4.0 * source
    traced = [None] * 7
    traced[0] = jnp.where(solid, q[0], hold * q[0] + level)
    for k, speed in ((1, ux), (3, uy), (5, uz)):
        shift = push * speed
        traced[k] = jnp.where(solid, q[k + 1], hold * q[k] + (level + shift))
        traced[k + 1] = jnp.where(solid, q[k], hold * q[k + 1] + (level - shift))

    rate = jnp.where(inflow, 1.0, rate)
    density = jnp.where(inflow, 1.0, density)
    ux, uy, uz = (jnp.where(inflow, w, u) for w, u in zip(wind, (ux, uy, uz)))
    rest = 1.0 - rate
    uxx, uyy, uzz = ux * ux, uy * uy, uz * uz
    base = rate * (density - 1.5 * (uxx + uyy + uzz))
    linear, quadratic = 3.0 * rate, 4.5 * rate
    lx, ly, lz = linear * ux, linear * uy, linear * uz
    qx, qy, qz = quadratic * uxx, quadratic * uyy, quadratic * uzz
    twice_x, twice_y = (linear * 3.0) * ux, (linear * 3.0) * uy
    cxy, cxz, cyz = twice_x * uy, twice_x * uz, twice_y * uz
    bx, by, bz = base + qx, base + qy, base + qz
    bxy, bxz, byz = bx + qy, bx + qz, by + qz
    relaxed = [None] * 19
    relaxed[0] = jnp.where(solid, h[0], rest * h[0] + base)
    parts = {
        1: (bx, lx),
        3: (by, ly),
        5: (bz, lz),
        7: (bxy + cxy, lx + ly),
        9: (bxy - cxy, lx - ly),
        11: (bxz + cxz, lx + lz),
        13: (bxz - cxz, lx - lz),
        15: (byz + cyz, ly + lz),
        17: (byz - cyz, ly - lz),
    }
    for k, (even, odd) in parts.items():
        relaxed[k] = jnp.where(solid, h[k + 1], rest * h[k] + (even + odd))
        relaxed[k + 1] = jnp.where(solid, h[k], rest * h[k + 1] + (even - odd))
    return relaxed + traced


def by_side(axis, body, near, far):
    even = lax.axis_index(axis) % 2 == 0
    pl.when(even)(lambda: body(near, far))
    pl.when(jnp.logical_not(even))(lambda: body(far, near))


def lane_index():
    return lax.broadcasted_iota(jnp.int32, (ROWS, LANES), 1)


def wind_tiles(wind):
    return [jnp.broadcast_to(wind[a : a + 1, :], (ROWS, LANES)) for a in range(3)]


def start_all(copies, sems):
    started = [pltpu.make_async_copy(src, dst, sems.at[n]) for n, (src, dst) in enumerate(copies)]
    for copy in started:
        copy.start()
    return started


def relax_own(cells, winds, store, rows):
    populations, tracer, solid, inflow, emission = cells
    h = [populations[k, rows, :] for k in range(FLOW)]
    q = [tracer[k, rows, :] for k in range(7)]
    built, held, emitted = solid[rows, :], inflow[rows, :], emission[rows, :]
    out = relax(h, q, built == 1, held == 1, emitted, winds)
    for u, value in enumerate(out + [built.astype(jnp.float32), held.astype(jnp.float32), emitted]):
        store(u, value)


def load_tiles(arrays, buffers, columns, sems, extra=()):
    copies = list(extra)
    for n, j in enumerate(columns):
        lanes = pl.ds(j * LANES, LANES)
        for array, buffer in zip(arrays, buffers):
            src = array.at[:, :, lanes] if len(array.shape) == 3 else array.at[:, lanes]
            copies.append((src, buffer.at[n]))
    started = start_all(copies, sems)
    count = len(arrays)
    own = [started[len(extra) + n * count : len(extra) + (n + 1) * count] for n in range(len(columns))]
    return started[: len(extra)], own


def first_edges(
    populations, tracer, solid, inflow, wind, emission, one, winds, y_near, y_far,
    wind_in, pop_in, tracer_in, solid_in, inflow_in, emission_in, sems,
):
    extent = populations.shape[1]
    tiles = populations.shape[2] // LANES
    nz = wind.shape[1]
    lane = lane_index()
    buffers = (pop_in, tracer_in, solid_in, inflow_in, emission_in)
    common, own = load_tiles(
        (populations, tracer, solid, inflow, emission), buffers, (tiles - 1, 0), sems, ((wind, wind_in),)
    )
    for copy in common:
        copy.wait()
    winds[...] = jnp.concatenate([wind_in[...]] * (LANES // nz), axis=1)
    wind_values = wind_tiles(winds)
    for n, at in enumerate((tiles, 1)):
        for copy in own[n]:
            copy.wait()
        cells = [b.at[n] for b in buffers]
        for r in range(0, extent, ROWS):
            rows = slice(r, r + ROWS)

            def keep(u, value, at=at, r=r):
                one[u, at, STEPS + r : STEPS + r + ROWS, :] = value

            relax_own(cells, wind_values, keep, rows)

    def pack(up, down):
        for at, sign, target in ((tiles, 1, up), (1, -1, down)):
            for r in range(0, extent, ROWS):
                def send(t, value, target=target, r=r):
                    target[t, r : r + ROWS, :] = value

                pack_columns(
                    lambda u, at=at, r=r: one[u, at, STEPS + r : STEPS + r + ROWS, :], send, sign, lane, nz
                )

    by_side("gy", pack, y_near, y_far)


def first_inner(
    populations, tracer, solid, inflow, emission, winds, _, one, x_near, x_far,
    pop_in, tracer_in, solid_in, inflow_in, emission_in, sems, *, nz,
):
    extent = populations.shape[1]
    tiles = populations.shape[2] // LANES
    height = lane_index() % nz
    buffers = (pop_in, tracer_in, solid_in, inflow_in, emission_in)
    columns = tuple(range(1, tiles - 1))
    _, own = load_tiles((populations, tracer, solid, inflow, emission), buffers, columns, sems)
    wind_values = wind_tiles(winds)

    for n, j in enumerate(columns):
        for copy in own[n]:
            copy.wait()
        for r in range(0, extent, ROWS):
            rows = slice(r, r + ROWS)

            def keep(u, value, j=j, r=r):
                one[u, j + 1, STEPS + r : STEPS + r + ROWS, :] = value

            relax_own([b.at[n] for b in buffers], wind_values, keep, rows)
    by_side("gx", lambda up, down: pack_sides(one, range(1, tiles + 1), up, down, extent, height), x_near, x_far)


def pack_sides(one, columns, up, down, extent, height):
    for at, c in enumerate(columns):
        for sign, target, first in ((1, up, extent), (-1, down, STEPS)):
            def store(offset, depth, value, target=target, at=at):
                target[at, offset : offset + depth, :] = value

            pack_rows(lambda u, low, depth, c=c: one[u, c, low : low + depth, :], store, sign, first, height)


def turn_corner(y_near, y_far, x_near, x_far, *, nz):
    extent = y_near.shape[1]
    height = lane_index() % nz

    def pack(sources, targets):
        for side, (sign_y, source) in enumerate(zip((1, -1), sources)):
            for sign, target, first in zip((1, -1), targets, (extent - STEPS, 0)):
                plan, (offset, row), (floor, roof), _ = corner_plan(sign, sign_y)
                for t, low, depth, at in plan:
                    target[side, at : at + depth, :] = source[t, first + low : first + low + depth, :]
                at = slice(first + row, first + row + 1)
                target[side, offset : offset + 1, :] = jnp.where(
                    height[:1] == 0, source[floor, at, :], source[roof, at, :]
                )

    by_side(
        "gy",
        lambda north, south: by_side("gx", lambda up, down: pack((south, north), (up, down)), x_near, x_far),
        y_near,
        y_far,
    )


def take_corners(one, near, far, stage, nz):
    wide, extent = one.shape[1], one.shape[2] - 2 * STEPS
    lane = lane_index()

    def lay(east, west):
        for side, sign_y in enumerate((1, -1)):
            for sign, source, first in ((1, west, 0), (-1, east, STEPS)):
                plan, (offset, row), walls, _ = corner_plan(sign, sign_y)
                for t, low, depth, at in plan:
                    stage[side, t, first + low : first + low + depth, :] = source[side, at : at + depth, :]
                for t in walls:
                    stage[side, t, first + row : first + row + 1, :] = source[side, offset : offset + 1, :]

    by_side("gx", lay, near, far)
    for side, (sign_y, c) in enumerate(((1, 0), (-1, wide - 1))):
        def store(u, value, c=c):
            one[u, c, :STEPS, :] = value[:STEPS]
            one[u, c, STEPS + extent :, :] = value[STEPS:]

        unpack_columns(lambda t, side=side: stage[side, t, :, :], store, sign_y, lane, nz)


class Mover:
    def __init__(self, nz):
        lane = lane_index()
        height = lane % nz
        self.nz = nz
        self.from_part = [None] + [lane >= part * nz for part in range(1, LANES // nz)]
        self.floor, self.roof = height == 0, height == nz - 1

    def merge(self, read, columns):
        value = read(columns[0])
        for part in range(1, len(columns)):
            if columns[part] != columns[part - 1]:
                value = jnp.where(self.from_part[part], read(columns[part]), value)
        return value

    def pull(self, read, parts, u):
        step_x, step_y, step_z = SPEED[u]
        value = self.merge(lambda c: read(u, c, step_x), parts[step_y])
        shift = (self.nz * step_y + step_z) % LANES
        if shift:
            value = pltpu.roll(value, shift, 1)
        if step_z:
            own = self.merge(lambda c: read(TURNED[u], c, 0), parts[0])
            value = jnp.where(self.floor if step_z == 1 else self.roof, own, value)
        return value


class Block:
    def __init__(self, one, two, three, four, done, winds, nz):
        self.levels = (None, one, two, three, four)
        self.done = done
        self.tiles = done.shape[1]
        self.extent = done.shape[2]
        self.last = self.tiles + 1
        self.both = self.tiles + 2
        self.count = LANES // nz
        self.mover = Mover(nz)
        self.winds = wind_tiles(winds)
        self.upper = lax.broadcasted_iota(jnp.int32, (ROWS, LANES), 0) < ROWS // 2

    def centre(self, step):
        low, high = STEPS + step, STEPS + self.extent - step
        return list(range(low, high - ROWS, ROWS)) + [high - ROWS]

    def seam(self, step):
        return (step, STEPS + self.extent - step)

    def read(self, level, u, c, place, back=0):
        ref = self.levels[level]
        if isinstance(place, tuple):
            low, high = place[0] - back, place[1] - back - ROWS // 2
            return jnp.where(self.upper, ref[u, c, low : low + ROWS, :], ref[u, c, high : high + ROWS, :])
        return ref[u, c, place - back : place - back + ROWS, :]

    def write(self, ref, u, c, place, value, lift=0):
        if isinstance(place, tuple):
            half = ROWS // 2
            ref[u, c, place[0] - lift : place[0] - lift + half, :] = value[:half]
            ref[u, c, place[1] - lift : place[1] - lift + half, :] = value[half:]
        else:
            ref[u, c, place - lift : place - lift + ROWS, :] = value

    def sources(self, level, c, before, after):
        tiles, last, both, count = self.tiles, self.last, self.both, self.count
        half = count // 2
        if c == both and level < 3:
            return {
                0: [last] * half + [0] * (count - half),
                1: [last] * (half - 1) + [0] * (count - half) + [tiles],
                -1: [1] + [last] * half + [0] * (count - half - 1),
            }
        return {0: [c] * count, 1: [c] * (count - 1) + [before], -1: [after] + [c] * (count - 1)}

    def around(self, level, c, margins):
        if not margins:
            return max(c - 1, 1), min(c + 1, self.tiles)
        if c == self.both:
            return self.tiles, 1
        before = self.both if c == 1 and level > 2 else max(c - 1, 0)
        after = self.both if c == self.tiles and level > 2 else min(c + 1, self.last)
        return before, after

    def pull(self, level, c, place, margins):
        parts = self.sources(level, c, *self.around(level, c, margins))
        return [
            self.mover.pull(lambda v, at, back: self.read(level, v, at, place, back), parts, u) for u in range(MOVING)
        ]

    def relax(self, step, c, place, margins):
        moved = self.pull(step, c, place, margins)
        here = self.sources(1, c, c, c)[0]
        solid, inflow, emission = (
            self.mover.merge(lambda at, u=u: self.read(1, u, at, place), here) for u in (SOLID, INFLOW, EMISSION)
        )
        out = relax(moved[:FLOW], moved[FLOW:], solid == 1.0, inflow == 1.0, emission, self.winds)
        for u in range(MOVING):
            self.write(self.levels[step + 1], u, c, place, out[u])

    def finish(self, c, place, margins):
        for u, value in enumerate(self.pull(STEPS, c, place, margins)):
            self.write(self.done, u, c - 1, place, value, STEPS)

    def steps(self, columns, places, margins):
        for step in range(1, STEPS):
            for c in columns(step):
                for place in places(step):
                    self.relax(step, c, place, margins)

    def inner(self, places):
        self.steps(lambda step: range(1, self.tiles + 1), places, False)
        for c in range(2, self.tiles):
            for place in places(STEPS):
                self.finish(c, place, False)

    def outer(self, places):
        self.steps(
            lambda step: (0, 1, self.tiles, self.last) if step == 1 else (self.both, 1, self.tiles), places, True
        )
        for c in (1, self.tiles):
            for place in places(STEPS):
                self.finish(c, place, True)


def inner_centre(winds, _, one, two, three, four, done, *, nz):
    block = Block(one, two, three, four, done, winds, nz)
    block.inner(block.centre)


def inner_seam(winds, near, far, *refs, nz):
    one, two, three, four, done = refs[5:]
    block = Block(one, two, three, four, done, winds, nz)
    columns = range(1, block.tiles + 1)
    by_side("gx", lambda east, west: fill_rows(one, columns, west, east, block.extent), near, far)
    block.inner(lambda step: [block.seam(step)])


def fill_rows(one, columns, west, east, extent):
    for at, c in enumerate(columns):
        for sign, source, first in ((1, west, 0), (-1, east, STEPS + extent)):
            def fill(u, row, value, c=c):
                one[u, c, row : row + value.shape[0], :] = value

            unpack_rows(
                lambda offset, depth, source=source, at=at: source[at, offset : offset + depth, :], fill, sign, first
            )


def outer_centre(winds, near, far, *refs, nz):
    one = refs[5]
    block = Block(*refs[5:], winds, nz)
    lane = lane_index()

    def unpack(north, south):
        for sign, source, c in ((1, south, 0), (-1, north, block.last)):
            for r in range(0, block.extent, ROWS):
                def store(u, value, c=c, r=r):
                    one[u, c, STEPS + r : STEPS + r + ROWS, :] = value

                unpack_columns(lambda t, source=source, r=r: source[t, r : r + ROWS, :], store, sign, lane, nz)

    by_side("gy", unpack, near, far)
    block.outer(block.centre)


def outer_seam(winds, near, far, *refs, nz):
    one, two, three, four, done, flow_out, tracer_out, stage, sems = refs[5:]
    block = Block(one, two, three, four, done, winds, nz)
    copies = []

    def write_out(j):
        lanes = pl.ds(j * LANES, LANES)
        for first, number, target in ((0, FLOW, flow_out), (FLOW, 7, tracer_out)):
            copy = pltpu.make_async_copy(
                done.at[pl.ds(first, number), j], target.at[:, :, lanes], sems.at[len(copies)]
            )
            copy.start()
            copies.append(copy)

    for j in range(1, block.tiles - 1):
        write_out(j)
    take_corners(one, near, far, stage, nz)
    block.steps(
        lambda step: (0, 1, block.tiles, block.last) if step == 1 else (block.both, 1, block.tiles),
        lambda step: [block.seam(step)],
        True,
    )
    for c in (1, block.tiles):
        block.finish(c, block.seam(STEPS), True)
        write_out(c - 1)
    for copy in copies:
        copy.wait()


def swapped(shard, axis, start):
    length = lax.axis_size(axis)
    pairs = [((i + start) % length, ((i ^ 1) + start) % length) for i in range(length)]
    return lax.ppermute(shard, axis, pairs)


def local(populations, tracer, solid_mask, inflow, wind_profile, emission):
    extent = populations.shape[1]
    tiles = populations.shape[2] // LANES
    nz = wind_profile.shape[1]
    inner_tiles = tiles - 2
    along, still, _ = split_units(1, 1)
    messages = len(along) + len(still)
    packed = row_plan(1)[2]
    rows = extent + 2 * STEPS
    vm = lambda *shape: pltpu.VMEM(shape, jnp.float32)
    far = pl.BlockSpec(memory_space=pltpu.HBM)
    close = pl.BlockSpec(memory_space=pltpu.VMEM)

    def buffers(number):
        return [
            vm(number, FLOW, extent, LANES),
            vm(number, 7, extent, LANES),
            pltpu.VMEM((number, extent, LANES), jnp.int32),
            pltpu.VMEM((number, extent, LANES), jnp.int32),
            vm(number, extent, LANES),
            pltpu.SemaphoreType.DMA((5 * number + 1,)),
        ]

    def run(body, out_shape, args, far_args=0, out_specs=None, scratch=(), aliases=None):
        specs = [far] * far_args + [close] * (len(args) - far_args)
        args = tuple(
            pltpu.with_memory_space_constraint(a, pltpu.HBM if n < far_args else pltpu.VMEM) for n, a in enumerate(args)
        )
        options = {} if out_specs is None else {"out_specs": out_specs}
        return pl.pallas_call(
            body,
            out_shape=out_shape,
            in_specs=specs,
            scratch_shapes=list(scratch),
            input_output_aliases=aliases or {},
            compiler_params=pltpu.CompilerParams(vmem_limit_bytes=KERNEL_BYTES),
            **options,
        )(*args)

    first = vm(UNITS, tiles + 2, rows, LANES)
    levels = (first, vm(MOVING, tiles + 2, rows, LANES)) + (vm(MOVING, tiles + 3, rows, LANES),) * 2
    levels += (vm(MOVING, tiles, extent, LANES),)
    one, winds, y_near, y_far = run(
        first_edges,
        (first, vm(3, LANES), vm(messages, extent, LANES), vm(messages, extent, LANES)),
        (populations, tracer, solid_mask, inflow, wind_profile, emission),
        far_args=6,
        scratch=[vm(3, nz)] + buffers(2),
    )
    y_near = swapped(y_near, "gy", 0)
    y_far = swapped(y_far, "gy", 1)
    one, x_near, x_far = run(
        lambda *refs: first_inner(*refs, nz=nz),
        (first, vm(tiles, packed, LANES), vm(tiles, packed, LANES)),
        (populations, tracer, solid_mask, inflow, emission, winds, one),
        far_args=5,
        scratch=buffers(inner_tiles),
        aliases={6: 0},
    )
    x_near = swapped(x_near, "gx", 0)
    x_far = swapped(x_far, "gx", 1)
    state = run(lambda *refs: inner_centre(*refs, nz=nz), levels, (winds, one), aliases={1: 0})
    turned = corner_plan(1, 1)[3]
    corner_near, corner_far = run(
        lambda *refs: turn_corner(*refs, nz=nz), (vm(2, turned, LANES), vm(2, turned, LANES)), (y_near, y_far)
    )
    corner_near = swapped(corner_near, "gx", 0)
    corner_far = swapped(corner_far, "gx", 1)
    state = run(
        lambda *refs: outer_centre(*refs, nz=nz),
        levels,
        (winds, y_near, y_far, *state),
        aliases={3 + n: n for n in range(5)},
    )
    state = run(
        lambda *refs: inner_seam(*refs, nz=nz),
        levels,
        (winds, x_near, x_far, *state),
        aliases={3 + n: n for n in range(5)},
    )
    out = run(
        lambda *refs: outer_seam(*refs, nz=nz),
        levels
        + (
            jax.ShapeDtypeStruct((FLOW, extent, tiles * LANES), jnp.float32),
            jax.ShapeDtypeStruct((7, extent, tiles * LANES), jnp.float32),
        ),
        (winds, corner_near, corner_far, *state),
        out_specs=(close,) * 5 + (far, far),
        scratch=[vm(2, messages, ROWS, LANES), pltpu.SemaphoreType.DMA((2 * tiles,))],
        aliases={3 + n: n for n in range(5)},
    )
    return out[5], out[6]


def solution(mesh):
    in_specs = (
        P(None, "gx", "gy"),
        P(None, "gx", "gy"),
        P("gx", "gy"),
        P("gx", "gy"),
        P(),
        P("gx", "gy"),
    )
    out_specs = (P(None, "gx", "gy"), P(None, "gx", "gy"))

    return jax.shard_map(local, mesh=mesh, in_specs=in_specs, out_specs=out_specs, check_vma=False)
```
